32 devices in a mesh: groups: 1, ep: 16 (over z, y, x), hp: 2 (over core).
Axes of the slice: x: 2, y: 2, z: 4, core: 2. Of those that a mesh axis runs over, the one named last changes fastest.
Arguments:
- x_pre: bfloat16 [896, 1536], P(('groups', 'ep')), may hold values from -6 to 6
- x_dec: bfloat16 [128, 1536], P(('groups', 'ep')), may hold values from -6 to 6
- prefill_query_rows: bfloat16 [896, 2048], P(('groups', 'ep'), 'hp'), may hold values from -240 to 240
- prefill_key_values: bfloat16 [2, 896, 256], P(None, ('groups', 'ep'), 'hp'), may hold values from -6.1 to 6.1
- decode_query_rows: bfloat16 [128, 2048], P(('groups', 'ep'), 'hp'), may hold values from -240 to 240
- decode_key_values: bfloat16 [2, 128, 256], P(None, ('groups', 'ep'), 'hp'), may hold values from -6 to 6
- cache: bfloat16 [2, 128, 128, 256], P(None, ('groups', 'ep'), None, 'hp'), may hold values from -6.1 to 6.1
- cache_len: int32 [128], P(('groups', 'ep')), may hold values from 2 to 128
- sinks: float32 [32], P('hp'), may hold values from -1 to 5
- o_weight: bfloat16 [2048, 1536], P('hp', 'ep'), may hold values from -0.125 to 0.125
- norm_gain: float32 [1536], replicated, may hold values from 0.5 to 1.5
- expert_ids: int32 [1024, 4], P(('groups', 'ep')), may hold values from 0 to 7, all different within a row; in each aligned block of 64 rows (0 to 63, 64 to 127, ...) at most 48 rows name the same one
- route_logits: float32 [1024, 4], P(('groups', 'ep')), may hold values from -6 to 6
- w_gate_up: bfloat16 [16, 2, 1536, 768], P('ep', None, None, 'hp'), may hold values from -0.15625 to 0.15625
- w_down: bfloat16 [16, 768, 1536], P('ep', 'hp'), may hold values from -0.15625 to 0.15625
Outputs:
- layer_out: bfloat16 [1024, 1536], P(('groups', 'ep', 'hp'))
The draws below stay inside these ranges and needn't reach their ends.
Inputs may be any that keep to these rules, and one draw needn't show every extreme that they name: `expert_ids`: each row names 4 different experts; among the rows of one index of ep no expert is named by more than 48 rows, and in every draw some expert is named by exactly 48 rows of some index.
All inputs are finite; a program needn't handle non-finite values.
Results may differ from the reference program's by a relative error of at most 0.0065.
Values may be sent and summed in bfloat16 or wider, within the bound.
No kernel may reach another device: no remote copies, remote signals or barrier semaphores. Data moves between devices by JAX's collectives and lax.ppermute only.
A program may use at most 64 MiB of HBM per device.

```python
import math
import jax
import jax.numpy as jnp
import numpy as np
from jax import lax

D = 1536
QUERY_HEADS = 32
LOCAL_KV_HEADS = 4
HEAD_SIZE = 64
FF = 1536
TOPK = 4
PREFILL_LOCAL = 56
DEC_DEV = 8
CACHE_POSITIONS = 128
EXPERTS = 8
PREFILL_TOKENS = 896
DECODE_COUNT = 128
TOK_DEV = 64
TOKENS = 1024
SLOT = 48
N_EP = 16


def prefill_index_pairs(key):
    base_offset = jax.random.normal(jax.random.fold_in(key, 11), (2, PREFILL_TOKENS, LOCAL_KV_HEADS * HEAD_SIZE), jnp.float32)
    return jnp.clip(base_offset, -6.1, 6.1)


def draw_prefill_key_values(key, part):
    return prefill_index_pairs(key).astype(jnp.bfloat16)


def draw_prefill_query_rows(key, part):
    base_offset = jnp.clip(jax.random.normal(jax.random.fold_in(key, 13), (PREFILL_TOKENS, QUERY_HEADS * HEAD_SIZE), jnp.float32), -6.0, 6.0)
    return jnp.clip(base_offset, -240.0, 240.0).astype(jnp.bfloat16)


def draw_cache(key, part):
    base_offset = jnp.clip(jax.random.normal(jax.random.fold_in(key, 22), (2, DECODE_COUNT, CACHE_POSITIONS, LOCAL_KV_HEADS * HEAD_SIZE), jnp.float32), -6.0, 6.0)
    return base_offset.astype(jnp.bfloat16)


def draw_decode_query_rows(key, part):
    base_offset = jnp.clip(jax.random.normal(jax.random.fold_in(key, 23), (DECODE_COUNT, QUERY_HEADS * HEAD_SIZE), jnp.float32), -6.0, 6.0)
    return jnp.clip(base_offset, -240.0, 240.0).astype(jnp.bfloat16)


def plant(values, key, smallest, top_value):
    shape = values.shape
    index_at = [jax.random.randint(jax.random.fold_in(key, axis), (), 0, shape[axis]) for axis in range(len(shape))]
    values = values.at[tuple(index_at)].set(smallest)
    longest = shape.index(max(shape))
    index_at[longest] = (index_at[longest] + 1) % shape[longest]
    return values.at[tuple(index_at)].set(top_value)


def shard_levels(stream_key, dims, pieces, least, largest):
    factor_of, own = 1.0, jax.random.fold_in(stream_key, 6)
    for axis_at, parts in pieces:
        draws = jnp.exp(jax.random.uniform(jax.random.fold_in(own, axis_at), (parts,), jnp.float32, least / len(pieces), largest / len(pieces)))
        factor_of = factor_of * jnp.repeat(draws, dims[axis_at] // parts).reshape([-1 if axis == axis_at else 1 for axis in range(len(dims))])
    return factor_of


def shared_out(key, own, number, rows, number_of, top, limit, lean):
    ranking = jax.random.permutation(key, number_of)
    heavy_load, ordinary = portions_of(number_of, rows * top, limit, lean, True), portions_of(number_of, rows * top, limit, lean, False)
    places = jnp.arange(number_of)

    def named(sizes, offset_by):
        used = int((sizes > 0).sum())
        fixed = max(1, used // 4)
        shifted = fixed + (places - fixed + offset_by * (used - fixed)) % max(1, number_of - fixed)
        return jnp.zeros((number_of,), jnp.int32).at[ranking[jnp.where(places < fixed, places, shifted)]].set(jnp.asarray(sizes, jnp.int32))

    sizes = jnp.where(number % 4 == 0, named(heavy_load, number // 4), named(ordinary, number - number // 4 - 1))
    mixed = jax.random.permutation(jax.random.fold_in(own, 3), number_of)
    giver, receiver = mixed[0:number_of // 2 * 2:2], mixed[1:number_of // 2 * 2:2]
    room = jnp.minimum(sizes[giver] - 1, limit - sizes[receiver]) // 2
    room = jnp.where((giver == ranking[0]) | (receiver == ranking[0]) | (sizes[receiver] == 0), 0, jnp.maximum(room, 0))
    shifted = jax.random.randint(jax.random.fold_in(own, 4), (number_of // 2,), 0, 1 << 20) % (room + 1)
    sizes = sizes.at[giver].add(-shifted).at[receiver].add(shifted)
    items = jnp.searchsorted(jnp.cumsum(sizes), jnp.arange(rows * top), side="right").astype(jnp.int32)
    grid = items.reshape(top, rows).T
    grid = grid[jax.random.permutation(jax.random.fold_in(own, 1), rows)]
    offset_by = jax.random.randint(jax.random.fold_in(own, 2), (rows, 1), 0, top)
    return jnp.take_along_axis(grid, (jnp.arange(top)[None, :] + offset_by) % top, axis=1)


def portions_of(number_of, total, most, skew, full):
    weights = [(1 << 20) // math.isqrt(rank ** skew) + 1 for rank in range(1, number_of + 1)]
    largest = most if full else min(most, max(-(-total // number_of), total * weights[0] // sum(weights)))
    least = 1 if total - largest >= number_of - 1 else 0
    given, spare = [largest] + [least] * (number_of - 1), total - largest - least * (number_of - 1)
    while spare > 0:
        candidates = [i for i in range(1, number_of) if given[i] < largest] or [i for i in range(1, number_of) if given[i] < most]
        whole, budget = sum([weights[i] for i in candidates]), spare
        for i in candidates:
            extra = min(most - given[i], max(1, budget * weights[i] // whole), spare)
            given[i] = given[i] + extra
            spare = spare - extra
    return np.array(given)


def centred(stream_key, extent, deviation, limit, split=(), held_as=jnp.bfloat16):
    array = deviation * jax.random.normal(stream_key, extent, jnp.float32)
    if split:
        array = array * shard_levels(stream_key, extent, split, -0.22, 0.18)
    return jnp.clip(array, -limit, limit).astype(held_as)


def setup_inputs(seed: int = 0, part: int = 0) -> dict:
    streams_of = jax.random.split(jax.random.key(seed), 16)
    part_keys = jax.random.split(jax.random.fold_in(streams_of[15], part), 16)
    x_pre = centred(part_keys[0], (PREFILL_TOKENS, D), 1.0, 6.0, ((0, 16),))
    x_dec = centred(part_keys[1], (DECODE_COUNT, D), 1.0, 6.0, ((0, 16),))
    prefill_query_rows = draw_prefill_query_rows(jax.random.fold_in(jax.random.fold_in(streams_of[15], part), 71), part)
    prefill_key_values = draw_prefill_key_values(jax.random.fold_in(jax.random.fold_in(streams_of[15], part), 71), part)
    decode_query_rows = draw_decode_query_rows(jax.random.fold_in(jax.random.fold_in(streams_of[15], part), 71), part)
    decode_key_values = centred(part_keys[5], (2, DECODE_COUNT, LOCAL_KV_HEADS * HEAD_SIZE), 1.0, 6.0, ((1, 16), (2, 2)))
    cache = draw_cache(jax.random.fold_in(jax.random.fold_in(streams_of[15], part), 71), part)
    cache_len = plant(jax.random.randint(part_keys[7], (DECODE_COUNT,), 2, CACHE_POSITIONS + 1), jax.random.fold_in(part_keys[7], 1), 2, CACHE_POSITIONS).astype(jnp.int32)
    sinks = jnp.clip(-1.0 + 6.0 * jax.random.uniform(streams_of[8], (QUERY_HEADS,), jnp.float32) ** shard_levels(streams_of[8], (QUERY_HEADS,), ((0, 2),), -0.2, 0.2), -1.0, 5.0)
    o_weight = centred(streams_of[9], (QUERY_HEADS * HEAD_SIZE, D), (QUERY_HEADS * HEAD_SIZE) ** -0.5, 0.125, ((0, 2), (1, 16)))
    norm_gain = jnp.clip(1.0 + 0.1 * jax.random.normal(streams_of[10], (D,), jnp.float32), 0.5, 1.5)
    expert_ids_keys = jax.random.split(jax.random.fold_in(part_keys[11], 1), TOKENS // TOK_DEV)
    expert_ids_turns = jax.random.permutation(jax.random.fold_in(part_keys[11], 3), TOKENS // TOK_DEV)
    expert_ids = jax.vmap(lambda own, number: shared_out(jax.random.fold_in(part_keys[11], 2), own, number, TOK_DEV, EXPERTS, TOPK, SLOT, 2))(expert_ids_keys, expert_ids_turns).reshape((TOKENS, TOPK))
    route_logits = centred(part_keys[12], (TOKENS, TOPK), 1.5, 6.0, ((0, 16),), jnp.float32)
    w_gate_up = centred(streams_of[13], (2 * EXPERTS, 2, D, FF // 2), D ** -0.5, 0.15625, ((0, 16), (3, 2)))
    w_down = centred(streams_of[14], (2 * EXPERTS, FF // 2, D), FF ** -0.5, 0.15625, ((0, 16), (1, 2)))
    return {"x_pre": x_pre, "x_dec": x_dec, "prefill_query_rows": prefill_query_rows, "prefill_key_values": prefill_key_values, "decode_query_rows": decode_query_rows, "decode_key_values": decode_key_values, "cache": cache, "cache_len": cache_len, "sinks": sinks, "o_weight": o_weight, "norm_gain": norm_gain, "expert_ids": expert_ids, "route_logits": route_logits, "w_gate_up": w_gate_up, "w_down": w_down}


EPS = 1e-05

def softmax_probability(scores, sink_logit_bias):
    top = jnp.maximum(lax.optimization_barrier(jnp.max(scores, axis=-1, keepdims=True)), sink_logit_bias)
    expo = jnp.exp(scores - top)
    total = lax.optimization_barrier(jnp.sum(expo, axis=-1, keepdims=True)) + jnp.exp(sink_logit_bias - top)
    return (expo / total).astype(jnp.bfloat16)

def prefill_attention(prefill_query_rows, prefill_key_values, sinks):
    head_group = QUERY_HEADS // LOCAL_KV_HEADS
    block_list = PREFILL_TOKENS // PREFILL_LOCAL
    key_rows = prefill_key_values[0].reshape(block_list, PREFILL_LOCAL, LOCAL_KV_HEADS, HEAD_SIZE)
    value_rows = prefill_key_values[1].reshape(block_list, PREFILL_LOCAL, LOCAL_KV_HEADS, HEAD_SIZE)
    query_rows = prefill_query_rows.reshape(block_list, PREFILL_LOCAL, LOCAL_KV_HEADS, head_group, HEAD_SIZE)
    sink_logit_bias = sinks.reshape(LOCAL_KV_HEADS, head_group)[None, :, :, None]
    places = jnp.arange(PREFILL_LOCAL, dtype=jnp.int32)
    visible = places[None, :] <= places[:, None]

    def one_block(args):
        rows, block_keys, block_values = args
        scores = jnp.einsum('qhgd,khd->qhgk', rows.astype(jnp.float32), block_keys.astype(jnp.float32)) * HEAD_SIZE ** (-0.5)
        scores = jnp.where(visible[:, None, None, :], scores, -jnp.inf)
        weight_matrix = softmax_probability(scores, sink_logit_bias)
        out = jnp.einsum('qhgk,khd->qhgd', weight_matrix.astype(jnp.float32), block_values.astype(jnp.float32))
        return out.astype(jnp.bfloat16).reshape(PREFILL_LOCAL, QUERY_HEADS * HEAD_SIZE)
    return lax.map(one_block, (query_rows, key_rows, value_rows)).reshape(PREFILL_TOKENS, QUERY_HEADS * HEAD_SIZE)

def decode_attention(decode_query_rows, decode_key_values, cache, cache_len, sinks):
    head_group = QUERY_HEADS // LOCAL_KV_HEADS
    query_rows = decode_query_rows.reshape(DECODE_COUNT, LOCAL_KV_HEADS, head_group, HEAD_SIZE).astype(jnp.float32)
    cached_key_rows = cache[0].reshape(DECODE_COUNT, CACHE_POSITIONS, LOCAL_KV_HEADS, HEAD_SIZE).astype(jnp.float32)
    cached_value_rows = cache[1].reshape(DECODE_COUNT, CACHE_POSITIONS, LOCAL_KV_HEADS, HEAD_SIZE).astype(jnp.float32)
    own_key_rows = decode_key_values[0].reshape(DECODE_COUNT, LOCAL_KV_HEADS, HEAD_SIZE).astype(jnp.float32)
    own_value_rows = decode_key_values[1].reshape(DECODE_COUNT, LOCAL_KV_HEADS, HEAD_SIZE).astype(jnp.float32)
    past_positions = jnp.einsum('shgd,sjhd->shgj', query_rows, cached_key_rows) * HEAD_SIZE ** (-0.5)
    live = jnp.arange(CACHE_POSITIONS, dtype=jnp.int32)[None, :] < cache_len[:, None]
    past_positions = jnp.where(live[:, None, None, :], past_positions, -jnp.inf)
    own_token = jnp.einsum('shgd,shd->shg', query_rows, own_key_rows)[..., None] * HEAD_SIZE ** (-0.5)
    weight_matrix = softmax_probability(jnp.concatenate([past_positions, own_token], axis=-1), sinks.reshape(LOCAL_KV_HEADS, head_group)[None, :, :, None])
    weight_matrix = weight_matrix.astype(jnp.float32)
    out = jnp.einsum('shgj,sjhd->shgd', weight_matrix[..., :CACHE_POSITIONS], cached_value_rows)
    out = out + weight_matrix[..., CACHE_POSITIONS:] * own_value_rows[:, :, None, :]
    return out.astype(jnp.bfloat16).reshape(DECODE_COUNT, QUERY_HEADS * HEAD_SIZE)

def device_major(pre, dec):
    first = pre.reshape(N_EP, PREFILL_LOCAL, pre.shape[-1])
    second = dec.reshape(N_EP, DEC_DEV, dec.shape[-1])
    return jnp.concatenate([first, second], axis=1).reshape(N_EP * (PREFILL_LOCAL + DEC_DEV), pre.shape[-1])

def reference(x_pre, x_dec, prefill_query_rows, prefill_key_values, decode_query_rows, decode_key_values, cache, cache_len, sinks, o_weight, norm_gain, expert_ids, route_logits, w_gate_up, w_down):
    attended = device_major(prefill_attention(prefill_query_rows, prefill_key_values, sinks), decode_attention(decode_query_rows, decode_key_values, cache, cache_len, sinks))
    stream = device_major(x_pre, x_dec).astype(jnp.float32) + jnp.dot(attended, o_weight, preferred_element_type=jnp.float32)
    mean_sq = lax.optimization_barrier(jnp.mean(stream * stream, axis=-1, keepdims=True))
    normed = (stream * lax.rsqrt(mean_sq + EPS) * norm_gain).astype(jnp.bfloat16)
    flat_ids = expert_ids.reshape(-1)
    capacity = N_EP * SLOT
    quarter = FF // 4

    def one_holder(outputs, args):
        expert, gate_up, down = args
        chosen = flat_ids == expert
        picked = jnp.nonzero(chosen, size=capacity, fill_value=0)[0].astype(jnp.int32)
        count = jnp.sum(chosen.astype(jnp.int32))
        live = (jnp.arange(capacity, dtype=jnp.int32) < count).astype(jnp.float32)
        rows = normed[picked // TOPK]
        gate = jnp.dot(rows, gate_up[0], preferred_element_type=jnp.float32)
        upper = jnp.dot(rows, gate_up[1], preferred_element_type=jnp.float32)
        hidden = ((upper + 1.0) * gate * jax.nn.sigmoid(1.702 * gate)).astype(jnp.bfloat16)
        lower_part = jnp.dot(hidden[:, :quarter], down[:quarter], preferred_element_type=jnp.float32).astype(jnp.bfloat16)
        upper_part = jnp.dot(hidden[:, quarter:], down[quarter:], preferred_element_type=jnp.float32).astype(jnp.bfloat16)
        lower_part, upper_part = lax.optimization_barrier((lower_part, upper_part))
        result = (lower_part.astype(jnp.float32) + upper_part.astype(jnp.float32)).astype(jnp.bfloat16)
        result = lax.optimization_barrier(result).astype(jnp.float32) * live[:, None]
        return (outputs.at[picked].add(result), None)
    holders = jnp.arange(2 * EXPERTS, dtype=jnp.int32) // 2
    outputs, _ = lax.scan(one_holder, jnp.zeros((TOKENS * TOPK, D), jnp.float32), (holders, w_gate_up, w_down))
    mix = jax.nn.softmax(route_logits, axis=-1)
    moe = lax.optimization_barrier(jnp.sum(outputs.reshape(TOKENS, TOPK, D) * mix[:, :, None], axis=1))
    return (stream + moe).astype(jnp.bfloat16)
```

```python
import jax
import jax.numpy as jnp
from jax import lax
from jax.sharding import PartitionSpec as P

HEAD_SIZE = 64


EPS = 1e-05


def softmax_probability(scores, sink_logit_bias):
    top = jnp.maximum(jnp.max(scores, axis=-1, keepdims=True), sink_logit_bias)
    expo = jnp.exp(scores - top)
    total = jnp.sum(expo, axis=-1, keepdims=True) + jnp.exp(sink_logit_bias - top)
    return (expo / total).astype(jnp.bfloat16)


def rms_norm(stream, gain):
    mean_sq = jnp.mean(stream * stream, axis=-1, keepdims=True)
    return (stream * lax.rsqrt(mean_sq + EPS) * gain).astype(jnp.bfloat16)


def attention(
    prefill_query_rows,
    prefill_key_values,
    decode_query_rows,
    decode_key_values,
    cache,
    cache_len,
    sinks,
):
    pre_rows = prefill_query_rows.shape[0]
    dec_rows = decode_query_rows.shape[0]
    kv_heads = prefill_key_values.shape[2] // HEAD_SIZE
    q_heads = sinks.shape[0]
    head_group = q_heads // kv_heads
    kv_max = cache.shape[2]
    scale = HEAD_SIZE ** (-0.5)
    sink_logit_bias = sinks.reshape(kv_heads, head_group)[None, :, :, None]
    keys_here = prefill_key_values[0].reshape(pre_rows, kv_heads, HEAD_SIZE)
    values_here = prefill_key_values[1].reshape(pre_rows, kv_heads, HEAD_SIZE)
    query_rows = prefill_query_rows.reshape(pre_rows, kv_heads, head_group, HEAD_SIZE)
    scores = (
        jnp.einsum("qhgd,khd->qhgk", query_rows, keys_here, preferred_element_type=jnp.float32)
        * scale
    )
    places = jnp.arange(pre_rows, dtype=jnp.int32)
    visible = places[None, :] <= places[:, None]
    scores = jnp.where(visible[:, None, None, :], scores, -jnp.inf)
    weight_matrix = softmax_probability(scores, sink_logit_bias)
    pre_out = jnp.einsum(
        "qhgk,khd->qhgd", weight_matrix, values_here, preferred_element_type=jnp.float32
    )
    pre_out = pre_out.astype(jnp.bfloat16).reshape(pre_rows, q_heads * HEAD_SIZE)
    dec_queries = decode_query_rows.reshape(dec_rows, kv_heads, head_group, HEAD_SIZE)
    cached_key_rows = cache[0].reshape(dec_rows, kv_max, kv_heads, HEAD_SIZE)
    cached_value_rows = cache[1].reshape(dec_rows, kv_max, kv_heads, HEAD_SIZE)
    own_key_rows = decode_key_values[0].reshape(dec_rows, kv_heads, HEAD_SIZE)
    own_value_rows = decode_key_values[1].reshape(dec_rows, kv_heads, HEAD_SIZE)
    past_positions = (
        jnp.einsum(
            "shgd,sjhd->shgj", dec_queries, cached_key_rows, preferred_element_type=jnp.float32
        )
        * scale
    )
    live = jnp.arange(kv_max, dtype=jnp.int32)[None, :] < cache_len[:, None]
    past_positions = jnp.where(live[:, None, None, :], past_positions, -jnp.inf)
    own_token = (
        jnp.einsum("shgd,shd->shg", dec_queries, own_key_rows, preferred_element_type=jnp.float32)[
            ..., None
        ]
        * scale
    )
    dec_weights = softmax_probability(
        jnp.concatenate([past_positions, own_token], axis=-1), sink_logit_bias
    )
    dec_out = jnp.einsum(
        "shgj,sjhd->shgd",
        dec_weights[..., :kv_max],
        cached_value_rows,
        preferred_element_type=jnp.float32,
    )
    dec_out = (
        dec_out
        + dec_weights[..., kv_max:].astype(jnp.float32)
        * own_value_rows.astype(jnp.float32)[:, :, None, :]
    )
    dec_out = dec_out.astype(jnp.bfloat16).reshape(dec_rows, q_heads * HEAD_SIZE)
    return jnp.concatenate([pre_out, dec_out], axis=0)


def slot_count(tokens_here, topk, experts):
    return min(
        tokens_here, 2 * ((3 * max(1, (tokens_here * topk + experts - 1) // experts) + 3) // 4)
    )


def slot_plan(
    attn_rows, resid, o_weight, norm_gain, expert_ids, route_logits, w_gate_up, w_down
):
    width = resid.shape[1]
    half = attn_rows.shape[0] // 2
    mine = lax.axis_index("hp") * half
    head_part = jnp.dot(
        attn_rows,
        lax.all_gather(o_weight, "ep", axis=1, tiled=True),
        preferred_element_type=jnp.float32,
    )
    summed = lax.psum_scatter(head_part, "hp", scatter_dimension=0, tiled=True)
    stream = lax.dynamic_slice_in_dim(resid, mine, half, 0).astype(jnp.float32) + summed
    normed = lax.all_gather(rms_norm(stream, norm_gain), "hp", axis=0, tiled=True)
    tokens_here, topk = expert_ids.shape
    holders = lax.axis_size("ep")
    experts = holders // 2
    slot = slot_count(tokens_here, topk, experts)
    plane = slot // 2
    flat_ids = expert_ids.reshape(-1)
    onehot = (flat_ids[:, None] == jnp.arange(experts, dtype=jnp.int32)[None, :]).astype(jnp.int32)
    rank = jnp.sum(jnp.cumsum(onehot, axis=0) * onehot, axis=1) - 1
    position = (flat_ids * slot + rank).reshape(tokens_here, topk)
    columns = jnp.arange(experts * slot, dtype=jnp.int32)[None, None, :] == position[:, :, None]
    picked_rows = jnp.any(columns, axis=1).T.astype(jnp.bfloat16)
    per_expert = (
        jnp.dot(picked_rows, normed, preferred_element_type=jnp.float32)
        .astype(jnp.bfloat16)
        .reshape(experts, slot, width)
    )
    send = jnp.repeat(per_expert, 2, axis=0)
    own_plane = lax.dynamic_slice_in_dim(send, lax.axis_index("hp") * plane, plane, 1)
    arrived_plane = lax.all_to_all(own_plane, "ep", split_axis=0, concat_axis=0, tiled=True)
    arrived = lax.all_gather(arrived_plane, "hp", axis=1, tiled=True)
    rows = arrived.reshape(-1, width)
    gate = jnp.dot(rows, w_gate_up[0, 0], preferred_element_type=jnp.float32)
    upper = jnp.dot(rows, w_gate_up[0, 1], preferred_element_type=jnp.float32)
    hidden = ((upper + 1.0) * gate * jax.nn.sigmoid(1.702 * gate)).astype(jnp.bfloat16)
    partial_out = jnp.dot(hidden, w_down[0], preferred_element_type=jnp.float32).reshape(
        -1, slot, width
    )
    share = lax.psum_scatter(
        partial_out.astype(jnp.bfloat16), "hp", scatter_dimension=1, tiled=True
    )
    returned = lax.all_to_all(share, "ep", split_axis=0, concat_axis=0, tiled=True)
    mix = jax.nn.softmax(route_logits, axis=-1)
    blend = jnp.sum(jnp.where(columns, mix[:, :, None], 0.0), axis=1).reshape(
        tokens_here, experts, slot
    )
    blend = jnp.repeat(blend, 2, axis=1)
    blend_plane = lax.dynamic_slice_in_dim(blend, lax.axis_index("hp") * plane, plane, 2).reshape(
        tokens_here, holders * plane
    )
    terms = jnp.dot(
        blend_plane,
        returned.reshape(-1, width).astype(jnp.float32),
        precision=lax.Precision.HIGHEST,
    )
    moe = lax.psum_scatter(
        terms.astype(jnp.bfloat16), "hp", scatter_dimension=0, tiled=True
    ).astype(jnp.float32)
    return (stream + moe).astype(jnp.bfloat16)


PLANE = 4


def plane_perm(holders, stage):
    return [
        (2 * e + h, 2 * (e ^ (1 if h == stage else 2)) + h) for e in range(holders) for h in (0, 1)
    ]


def line_perm(holders, step):
    return [(e, (e + PLANE * step) % holders) for e in range(holders)]


def at(blocks, index):
    return lax.dynamic_index_in_dim(blocks, index, 0, keepdims=False)


def dense_plan(
    attn_rows, resid, o_weight, norm_gain, expert_ids, route_logits, w_gate_up, w_down
):
    tokens_here, width = resid.shape
    holders = lax.axis_size("ep")
    experts = holders // 2
    deep = holders // PLANE
    place, core = lax.axis_index("ep"), lax.axis_index("hp")
    line, spot = place // PLANE, place % PLANE
    half = tokens_here // 2
    swap = [(0, 1), (1, 0)]
    far_first = range(deep - 1, 0, -1)

    def plane(value, stage):
        return lax.ppermute(value, ("ep", "hp"), plane_perm(holders, stage))

    def along(value, step):
        return lax.ppermute(value, "ep", line_perm(holders, step))

    def gather_line(value):
        blocks = {0: value, **{k: along(value, k) for k in far_first}}
        near = jnp.stack([blocks[k] for k in range(deep)])
        return [at(near, (line - c) % deep) for c in range(deep)]

    gate_up_here, down_here = w_gate_up[0], w_down[0]
    gate_up_there = lax.ppermute(gate_up_here, "hp", swap)
    down_there = lax.ppermute(down_here, "hp", swap)

    columns = o_weight.T
    beside = plane(columns, 0)
    across = plane(jnp.stack([columns, beside]), 1)
    near = jnp.stack([columns, beside, across[0], across[1]])
    bits = [spot ^ q for q in range(PLANE)]
    near_at = [jnp.where(core == 0, d, (d >> 1) | ((d & 1) << 1)) for d in bits]
    weight = jnp.concatenate([at(near, j) for j in near_at], axis=0)

    mix = jax.nn.softmax(route_logits, axis=-1)
    chosen = expert_ids[:, :, None] == jnp.arange(experts, dtype=jnp.int32)[None, None, :]
    factor = jnp.sum(jnp.where(chosen, mix[:, :, None], 0.0), axis=1)
    high = factor.astype(jnp.bfloat16)
    low = (factor - high.astype(jnp.float32)).astype(jnp.bfloat16)
    pad = -2 * experts % 128
    tail = jnp.concatenate(
        [high, low] + ([jnp.zeros((tokens_here, pad), jnp.bfloat16)] if pad else []), axis=1
    )
    own_rows = lax.dynamic_slice_in_dim(
        jnp.concatenate([resid, tail], axis=1), core * half, half, 0
    )

    rows = jnp.concatenate(gather_line(attn_rows), axis=0)
    wide = jnp.concatenate(gather_line(own_rows), axis=0)
    part = lax.dot_general(
        rows, weight, (((1,), (1,)), ((), ())), preferred_element_type=jnp.float32
    ).reshape(deep, tokens_here, -1)
    kept = lax.dynamic_slice_in_dim(part, core * half, half, 1)
    given = lax.dynamic_slice_in_dim(part, (1 - core) * half, half, 1)
    summed = (kept + lax.ppermute(given, "hp", swap)).astype(jnp.bfloat16)
    attended = jnp.concatenate(
        [block.reshape(deep * half, -1) for block in gather_line(summed)], axis=1
    )
    stream = wide[:, :width].astype(jnp.float32) + attended.astype(jnp.float32)
    tokens = jnp.concatenate([rms_norm(stream, norm_gain), wide[:, width:]], axis=1)
    own_stream = lax.dynamic_slice_in_dim(stream, line * half, half, 0)

    mine = place // 2

    def expert(block):
        inputs, tail = block[:, :width], block[:, width:].astype(jnp.float32)
        lanes = jnp.arange(tail.shape[1], dtype=jnp.int32)[None, :]
        scale = jnp.sum(
            jnp.where((lanes == mine) | (lanes == mine + experts), tail, 0.0), 1, keepdims=True
        )
        total = 0.0
        for gate_up, down in ((gate_up_here, down_here), (gate_up_there, down_there)):
            gate = jnp.dot(inputs, gate_up[0], preferred_element_type=jnp.float32)
            upper = jnp.dot(inputs, gate_up[1], preferred_element_type=jnp.float32)
            hidden = ((upper + 1.0) * gate * jax.nn.sigmoid(1.702 * gate)).astype(jnp.bfloat16)
            total = total + jnp.dot(hidden, down, preferred_element_type=jnp.float32)
        return total * scale

    count = tokens.shape[0]
    near_tokens = plane(tokens, 0)
    far_tokens = plane(jnp.concatenate([tokens, near_tokens]), 1)
    first = expert(jnp.concatenate([tokens, near_tokens]))
    last = expert(far_tokens[count:])
    third = expert(far_tokens[:count])
    back = plane(
        jnp.concatenate([first[count:].astype(jnp.bfloat16), last.astype(jnp.bfloat16)]), 0
    )
    over = plane((third + back[count:].astype(jnp.float32)).astype(jnp.bfloat16), 1)
    moe = first[:count] + back[:count].astype(jnp.float32) + over.astype(jnp.float32)
    moe = moe.reshape(deep, half, width)
    sent = moe.astype(jnp.bfloat16)
    got = [along(at(sent, (line + k) % deep), k) for k in far_first]
    total = own_stream + at(moe, line)
    for block in got:
        total = total + block.astype(jnp.float32)
    return total.astype(jnp.bfloat16)


def on_device(
    x_pre,
    x_dec,
    prefill_query_rows,
    prefill_key_values,
    decode_query_rows,
    decode_key_values,
    cache,
    cache_len,
    sinks,
    o_weight,
    norm_gain,
    expert_ids,
    route_logits,
    w_gate_up,
    w_down,
):
    attn_rows = attention(
        prefill_query_rows,
        prefill_key_values,
        decode_query_rows,
        decode_key_values,
        cache,
        cache_len,
        sinks,
    )
    resid = jnp.concatenate([x_pre, x_dec], axis=0)
    rest = (attn_rows, resid, o_weight, norm_gain, expert_ids, route_logits, w_gate_up, w_down)
    tokens_here, topk = expert_ids.shape
    holders = lax.axis_size("ep")
    dense = tokens_here <= 2 * slot_count(tokens_here, topk, holders // 2)
    if dense and holders % PLANE == 0 and holders > PLANE and lax.axis_size("hp") == 2:
        return dense_plan(*rest)
    return slot_plan(*rest)


def solution(mesh):
    placed = (
        P(("groups", "ep"), None),
        P(("groups", "ep"), None),
        P(("groups", "ep"), "hp"),
        P(None, ("groups", "ep"), "hp"),
        P(("groups", "ep"), "hp"),
        P(None, ("groups", "ep"), "hp"),
        P(None, ("groups", "ep"), None, "hp"),
        P(("groups", "ep")),
        P("hp"),
        P("hp", "ep"),
        P(),
        P(("groups", "ep"), None),
        P(("groups", "ep"), None),
        P("ep", None, None, "hp"),
        P("ep", "hp", None),
    )
    return jax.shard_map(
        on_device,
        mesh=mesh,
        in_specs=placed,
        out_specs=P(("groups", "ep", "hp"), None),
        check_vma=False,
    )
```

```python
import functools
import jax
import jax.numpy as jnp
from jax import lax
from jax.experimental import pallas as pl
from jax.experimental.pallas import tpu as pltpu
from jax.sharding import PartitionSpec as P

HEAD_SIZE = 64


EPS = 1e-05


def rms_norm(stream, gain):
    mean_sq = jnp.mean(stream * stream, axis=-1, keepdims=True)
    return (stream * lax.rsqrt(mean_sq + EPS) * gain).astype(jnp.bfloat16)


def attention_kernel(
    sinks_ref, len_ref, pre_q_ref, pre_kv_ref, dec_q_ref, dec_kv_ref, cache_ref, out_ref
):
    pre_rows, q_width = pre_q_ref.shape
    dec_rows = dec_q_ref.shape[0]
    lanes = 2 * HEAD_SIZE
    pairs = q_width // lanes
    group = (q_width // HEAD_SIZE) // (pre_kv_ref.shape[2] // HEAD_SIZE)
    scale = HEAD_SIZE ** (-0.5)
    padded = -(-pre_rows // 16) * 16
    positions = cache_ref.shape[2]

    def lane(rows):
        return lax.broadcasted_iota(jnp.int32, (rows, lanes), 1)

    def aligned(pair, side, head, rows):
        value = pair if side == head % 2 else pltpu.roll(pair, HEAD_SIZE, 1)
        return jnp.where((lane(rows) // HEAD_SIZE) == head % 2, value, 0.0)

    def joined(low, high, head, rows):
        low = low if head % 2 == 0 else pltpu.roll(low, HEAD_SIZE, 1)
        high = high if head % 2 == 1 else pltpu.roll(high, HEAD_SIZE, 1)
        return jnp.where(lane(rows) < HEAD_SIZE, low, high)

    def weights(scores, sink, more=None):
        top = jnp.maximum(jnp.max(scores, axis=-1, keepdims=True), sink)
        if more is not None:
            top = jnp.maximum(top, more)
        expo = jnp.exp(scores - top)
        total = jnp.sum(expo, axis=-1, keepdims=True) + jnp.exp(sink - top)
        if more is None:
            return (expo / total).astype(jnp.bfloat16), None
        extra = jnp.exp(more - top)
        total = total + extra
        return (expo / total).astype(jnp.bfloat16), (extra / total).astype(jnp.bfloat16)

    def filled(value):
        return jnp.concatenate(
            [value.astype(jnp.float32), jnp.zeros((padded - pre_rows, lanes), jnp.float32)], 0
        ).astype(jnp.bfloat16)

    contract = (((1,), (1,)), ((), ()))
    key_at = lax.broadcasted_iota(jnp.int32, (pre_rows, padded), 1)
    visible = key_at <= lax.broadcasted_iota(jnp.int32, (pre_rows, padded), 0)
    row_seq = lax.broadcasted_iota(jnp.int32, (dec_rows, positions), 0)
    length = jnp.zeros((dec_rows, positions), jnp.int32)
    for s in range(dec_rows):
        length = jnp.where(row_seq == s, len_ref[s], length)
    live = lax.broadcasted_iota(jnp.int32, (dec_rows, positions), 1) < length

    for head in range(pre_kv_ref.shape[2] // HEAD_SIZE):
        at_lanes = pl.ds((head // 2) * lanes, lanes)
        first_pair = head * group // 2
        here = range(first_pair, first_pair + group // 2)
        stacked = []
        for p in here:
            pair = pre_q_ref[:, pl.ds(p * lanes, lanes)].astype(jnp.float32)
            stacked += [aligned(pair, side, head, pre_rows) for side in (0, 1)]
        queries = jnp.concatenate(stacked, axis=0).astype(jnp.bfloat16)
        keys = filled(pre_kv_ref[0, :, at_lanes])
        scores = lax.dot_general(queries, keys, contract, preferred_element_type=jnp.float32)
        probs = []
        for i in range(group):
            block = scores[i * pre_rows : (i + 1) * pre_rows] * scale
            block = jnp.where(visible, block, -jnp.inf)
            probs.append(weights(block, sinks_ref[head * group + i])[0].astype(jnp.float32))
        pre_out = jnp.dot(
            jnp.concatenate(probs, axis=0).astype(jnp.bfloat16),
            filled(pre_kv_ref[1, :, at_lanes]),
            preferred_element_type=jnp.float32,
        )
        stacked = []
        for p in here:
            pair = dec_q_ref[:, pl.ds(p * lanes, lanes)].astype(jnp.float32)
            stacked += [aligned(pair, side, head, dec_rows) for side in (0, 1)]
        flat = jnp.concatenate(stacked, axis=0)
        queries = flat.astype(jnp.bfloat16)
        owner = lax.broadcasted_iota(jnp.int32, (group * dec_rows, positions), 0) % dec_rows
        past = jnp.zeros((group * dec_rows, positions), jnp.float32)
        for s in range(dec_rows):
            block = lax.dot_general(
                queries, cache_ref[0, s, :, at_lanes], contract, preferred_element_type=jnp.float32
            )
            past = jnp.where(owner == s, block, past)
        own_keys = dec_kv_ref[0, :, at_lanes].astype(jnp.float32)
        own_values = dec_kv_ref[1, :, at_lanes].astype(jnp.float32)
        probs, extras = [], []
        for i in range(group):
            rows = slice(i * dec_rows, (i + 1) * dec_rows)
            block = jnp.where(live, past[rows] * scale, -jnp.inf)
            own = jnp.sum(flat[rows] * own_keys, axis=1, keepdims=True) * scale
            prob, extra = weights(block, sinks_ref[head * group + i], own)
            probs.append(prob.astype(jnp.float32))
            extras.append(extra.astype(jnp.float32) * own_values)
        probs = jnp.concatenate(probs, axis=0)
        dec_out = jnp.concatenate(extras, axis=0)
        for s in range(dec_rows):
            dec_out = dec_out + jnp.dot(
                jnp.where(owner == s, probs, 0.0).astype(jnp.bfloat16),
                cache_ref[1, s, :, at_lanes],
                preferred_element_type=jnp.float32,
            )
        for n, p in enumerate(here):
            low, high = 2 * n, 2 * n + 1
            pre_pair = joined(
                pre_out[low * pre_rows : (low + 1) * pre_rows],
                pre_out[high * pre_rows : (high + 1) * pre_rows],
                head,
                pre_rows,
            )
            dec_pair = joined(
                dec_out[low * dec_rows : (low + 1) * dec_rows],
                dec_out[high * dec_rows : (high + 1) * dec_rows],
                head,
                dec_rows,
            )
            out_ref[:, pl.ds(p * lanes, lanes)] = jnp.concatenate([pre_pair, dec_pair], 0).astype(
                out_ref.dtype
            )


def attention(
    prefill_query_rows,
    prefill_key_values,
    decode_query_rows,
    decode_key_values,
    cache,
    cache_len,
    sinks,
):
    rows = prefill_query_rows.shape[0] + decode_query_rows.shape[0]
    width = prefill_query_rows.shape[1]
    scalars = pl.BlockSpec(memory_space=pltpu.SMEM)
    vectors = pl.BlockSpec(memory_space=pltpu.VMEM)
    return pl.pallas_call(
        attention_kernel,
        out_shape=jax.ShapeDtypeStruct((rows, width), jnp.bfloat16),
        in_specs=[scalars] * 2 + [vectors] * 5,
        out_specs=vectors,
        cost_estimate=pl.CostEstimate(
            flops=4_000_000_000, bytes_accessed=1_000_000, transcendentals=200_000
        ),
        compiler_params=pltpu.CompilerParams(vmem_limit_bytes=16 * 2**20),
        name="attention",
    )(
        sinks,
        cache_len,
        prefill_query_rows,
        prefill_key_values,
        decode_query_rows,
        decode_key_values,
        cache,
    )


def slot_count(tokens_here, topk, experts):
    return min(
        tokens_here, 2 * ((3 * max(1, (tokens_here * topk + experts - 1) // experts) + 3) // 4)
    )


def slot_plan(
    attn_rows, resid, o_weight, norm_gain, expert_ids, route_logits, w_gate_up, w_down
):
    width = resid.shape[1]
    half = attn_rows.shape[0] // 2
    mine = lax.axis_index("hp") * half
    head_part = jnp.dot(
        attn_rows,
        lax.all_gather(o_weight, "ep", axis=1, tiled=True),
        preferred_element_type=jnp.float32,
    )
    summed = lax.psum_scatter(head_part, "hp", scatter_dimension=0, tiled=True)
    stream = lax.dynamic_slice_in_dim(resid, mine, half, 0).astype(jnp.float32) + summed
    normed = lax.all_gather(rms_norm(stream, norm_gain), "hp", axis=0, tiled=True)
    tokens_here, topk = expert_ids.shape
    holders = lax.axis_size("ep")
    experts = holders // 2
    slot = slot_count(tokens_here, topk, experts)
    plane = slot // 2
    flat_ids = expert_ids.reshape(-1)
    onehot = (flat_ids[:, None] == jnp.arange(experts, dtype=jnp.int32)[None, :]).astype(jnp.int32)
    rank = jnp.sum(jnp.cumsum(onehot, axis=0) * onehot, axis=1) - 1
    position = (flat_ids * slot + rank).reshape(tokens_here, topk)
    columns = jnp.arange(experts * slot, dtype=jnp.int32)[None, None, :] == position[:, :, None]
    picked_rows = jnp.any(columns, axis=1).T.astype(jnp.bfloat16)
    per_expert = (
        jnp.dot(picked_rows, normed, preferred_element_type=jnp.float32)
        .astype(jnp.bfloat16)
        .reshape(experts, slot, width)
    )
    send = jnp.repeat(per_expert, 2, axis=0)
    own_plane = lax.dynamic_slice_in_dim(send, lax.axis_index("hp") * plane, plane, 1)
    arrived_plane = lax.all_to_all(own_plane, "ep", split_axis=0, concat_axis=0, tiled=True)
    arrived = lax.all_gather(arrived_plane, "hp", axis=1, tiled=True)
    rows = arrived.reshape(-1, width)
    gate = jnp.dot(rows, w_gate_up[0, 0], preferred_element_type=jnp.float32)
    upper = jnp.dot(rows, w_gate_up[0, 1], preferred_element_type=jnp.float32)
    hidden = ((upper + 1.0) * gate * jax.nn.sigmoid(1.702 * gate)).astype(jnp.bfloat16)
    partial_out = jnp.dot(hidden, w_down[0], preferred_element_type=jnp.float32).reshape(
        -1, slot, width
    )
    share = lax.psum_scatter(
        partial_out.astype(jnp.bfloat16), "hp", scatter_dimension=1, tiled=True
    )
    returned = lax.all_to_all(share, "ep", split_axis=0, concat_axis=0, tiled=True)
    mix = jax.nn.softmax(route_logits, axis=-1)
    blend = jnp.sum(jnp.where(columns, mix[:, :, None], 0.0), axis=1).reshape(
        tokens_here, experts, slot
    )
    blend = jnp.repeat(blend, 2, axis=1)
    blend_plane = lax.dynamic_slice_in_dim(blend, lax.axis_index("hp") * plane, plane, 2).reshape(
        tokens_here, holders * plane
    )
    terms = jnp.dot(
        blend_plane,
        returned.reshape(-1, width).astype(jnp.float32),
        precision=lax.Precision.HIGHEST,
    )
    moe = lax.psum_scatter(
        terms.astype(jnp.bfloat16), "hp", scatter_dimension=0, tiled=True
    ).astype(jnp.float32)
    return (stream + moe).astype(jnp.bfloat16)


def expert_kernel(mine_ref, rows_ref, gate_up_a, gate_up_b, down_a, down_b, out_ref, *, experts):
    width = gate_up_a.shape[1]
    inputs = rows_ref[:, :width]
    tail = rows_ref[:, width:].astype(jnp.float32)
    lanes = lax.broadcasted_iota(jnp.int32, tail.shape, 1)
    mine = mine_ref[0]
    scale = jnp.sum(
        jnp.where((lanes == mine) | (lanes == mine + experts), tail, 0.0), 1, keepdims=True
    )
    total = None
    for gate_up, down in ((gate_up_a, down_a), (gate_up_b, down_b)):
        gate = jnp.dot(inputs, gate_up[0], preferred_element_type=jnp.float32)
        upper = jnp.dot(inputs, gate_up[1], preferred_element_type=jnp.float32)
        hidden = ((upper + 1.0) * gate * jax.nn.sigmoid(1.702 * gate)).astype(jnp.bfloat16)
        part = jnp.dot(hidden, down[...], preferred_element_type=jnp.float32)
        total = part if total is None else total + part
    out_ref[...] = (total * scale).astype(out_ref.dtype)


def expert_rows(mine, rows, weights, experts, out_type):
    count, width, units = rows.shape[0], weights[0].shape[1], 2 * weights[0].shape[2]
    vectors = pl.BlockSpec(memory_space=pltpu.VMEM)
    return pl.pallas_call(
        functools.partial(expert_kernel, experts=experts),
        out_shape=jax.ShapeDtypeStruct((count, width), out_type),
        in_specs=[pl.BlockSpec(memory_space=pltpu.SMEM)] + [vectors] * 5,
        out_specs=vectors,
        cost_estimate=pl.CostEstimate(
            flops=6 * count * width * units,
            bytes_accessed=6 * width * units,
            transcendentals=count * units,
        ),
        compiler_params=pltpu.CompilerParams(vmem_limit_bytes=24 * 2**20),
        name="expert",
    )(mine, rows, *weights)


PLANE = 4


def plane_perm(holders, stage):
    return [
        (2 * e + h, 2 * (e ^ (1 if h == stage else 2)) + h) for e in range(holders) for h in (0, 1)
    ]


def line_perm(holders, step):
    return [(e, (e + PLANE * step) % holders) for e in range(holders)]


def at(blocks, index):
    return lax.dynamic_index_in_dim(blocks, index, 0, keepdims=False)


def dense_plan(
    attn_rows, resid, o_weight, norm_gain, expert_ids, route_logits, w_gate_up, w_down
):
    tokens_here, width = resid.shape
    holders = lax.axis_size("ep")
    experts = holders // 2
    deep = holders // PLANE
    place, core = lax.axis_index("ep"), lax.axis_index("hp")
    line, spot = place // PLANE, place % PLANE
    half = tokens_here // 2
    swap = [(0, 1), (1, 0)]
    far_first = range(deep - 1, 0, -1)

    def plane(value, stage):
        return lax.ppermute(value, ("ep", "hp"), plane_perm(holders, stage))

    def along(value, step):
        return lax.ppermute(value, "ep", line_perm(holders, step))

    def in_order(blocks):
        near = jnp.stack(blocks)
        return [at(near, (line - c) % deep) for c in range(deep)]

    def gather_line(value):
        got = {k: along(value, k) for k in far_first}
        return in_order([value] + [got[k] for k in range(1, deep)])

    gate_up_here, down_here = w_gate_up[0], w_down[0]
    gate_up_there = lax.ppermute(gate_up_here, "hp", swap)
    down_there = lax.ppermute(down_here, "hp", swap)
    weights = (gate_up_here, gate_up_there, down_here, down_there)

    columns = o_weight.T
    beside = plane(columns, 0)
    across = plane(jnp.stack([columns, beside]), 1)
    near = jnp.stack([columns, beside, across[0], across[1]])
    bits = [spot ^ q for q in range(PLANE)]
    near_at = [jnp.where(core == 0, d, (d >> 1) | ((d & 1) << 1)) for d in bits]
    weight = jnp.concatenate([at(near, j) for j in near_at], axis=0)

    rows = jnp.concatenate(gather_line(attn_rows), axis=0)

    mix = jax.nn.softmax(route_logits, axis=-1)
    chosen = expert_ids[:, :, None] == jnp.arange(experts, dtype=jnp.int32)[None, None, :]
    factor = jnp.sum(jnp.where(chosen, mix[:, :, None], 0.0), axis=1)
    high = factor.astype(jnp.bfloat16)
    low = (factor - high.astype(jnp.float32)).astype(jnp.bfloat16)
    pad = -2 * experts % 128
    tail = jnp.concatenate(
        [high, low] + ([jnp.zeros((tokens_here, pad), jnp.bfloat16)] if pad else []), axis=1
    )
    share = width // deep
    own_rows = lax.dynamic_slice_in_dim(resid, core * half, half, 0)
    own_tail = lax.dynamic_slice_in_dim(tail, core * half, half, 0)

    def addressed(k):
        piece = lax.dynamic_slice_in_dim(own_rows, ((line + k) % deep) * share, share, 1)
        return jnp.concatenate([piece, own_tail], axis=1)

    arrived = {k: along(addressed(k), k) for k in far_first}
    arrived[0] = addressed(0)
    arrived = jnp.stack(in_order([arrived[k] for k in range(deep)]))
    tails = arrived[:, :, share:].reshape(deep * half, -1)

    part = lax.dot_general(
        rows, weight, (((1,), (1,)), ((), ())), preferred_element_type=jnp.float32
    ).reshape(deep, tokens_here, -1)
    kept = lax.dynamic_slice_in_dim(part, core * half, half, 1)
    given = lax.dynamic_slice_in_dim(part, (1 - core) * half, half, 1)
    summed = kept + lax.ppermute(given, "hp", swap) + arrived[:, :, :share].astype(jnp.float32)
    stream = jnp.concatenate(
        [block.reshape(deep * half, -1) for block in gather_line(summed.astype(jnp.bfloat16))],
        axis=1,
    ).astype(jnp.float32)
    tokens = jnp.concatenate([rms_norm(stream, norm_gain), tails], axis=1)
    own_stream = lax.dynamic_slice_in_dim(stream, line * half, half, 0)

    mine = jnp.reshape(place // 2, (1,))

    def expert(block, out_type):
        return expert_rows(mine, block, weights, experts, out_type)

    near_tokens = plane(tokens, 0)
    both_tokens = plane(near_tokens, 1)
    far_tokens = plane(tokens, 1)
    own = expert(tokens, jnp.float32)
    near_out = expert(near_tokens, jnp.bfloat16)
    both_out = expert(both_tokens, jnp.bfloat16)
    far_out = expert(far_tokens, jnp.float32)
    far_back = plane(both_out, 0)
    near_back = plane(near_out, 0)
    over = plane((far_out + far_back.astype(jnp.float32)).astype(jnp.bfloat16), 1)
    moe = own + near_back.astype(jnp.float32) + over.astype(jnp.float32)
    moe = moe.reshape(deep, half, width)
    sent = moe.astype(jnp.bfloat16)
    got = [along(at(sent, (line + k) % deep), k) for k in far_first]
    total = own_stream + at(moe, line)
    for block in got:
        total = total + block.astype(jnp.float32)
    return total.astype(jnp.bfloat16)


def on_device(
    x_pre,
    x_dec,
    prefill_query_rows,
    prefill_key_values,
    decode_query_rows,
    decode_key_values,
    cache,
    cache_len,
    sinks,
    o_weight,
    norm_gain,
    expert_ids,
    route_logits,
    w_gate_up,
    w_down,
):
    attn_rows = attention(
        prefill_query_rows,
        prefill_key_values,
        decode_query_rows,
        decode_key_values,
        cache,
        cache_len,
        sinks,
    )
    resid = jnp.concatenate([x_pre, x_dec], axis=0)
    rest = (attn_rows, resid, o_weight, norm_gain, expert_ids, route_logits, w_gate_up, w_down)
    tokens_here, topk = expert_ids.shape
    holders = lax.axis_size("ep")
    dense = tokens_here <= 2 * slot_count(tokens_here, topk, holders // 2)
    if dense and resid.shape[1] % (holders // PLANE * 128) == 0 and holders % PLANE == 0 and holders > PLANE and lax.axis_size("hp") == 2:
        return dense_plan(*rest)
    return slot_plan(*rest)


def solution(mesh):
    placed = (
        P(("groups", "ep"), None),
        P(("groups", "ep"), None),
        P(("groups", "ep"), "hp"),
        P(None, ("groups", "ep"), "hp"),
        P(("groups", "ep"), "hp"),
        P(None, ("groups", "ep"), "hp"),
        P(None, ("groups", "ep"), None, "hp"),
        P(("groups", "ep")),
        P("hp"),
        P("hp", "ep"),
        P(),
        P(("groups", "ep"), None),
        P(("groups", "ep"), None),
        P("ep", None, None, "hp"),
        P("ep", "hp", None),
    )
    return jax.shard_map(
        on_device,
        mesh=mesh,
        in_specs=placed,
        out_specs=P(("groups", "ep", "hp"), None),
        check_vma=False,
    )
```

```python
import functools
import jax
import jax.numpy as jnp
from jax import lax
from jax.experimental import pallas as pl
from jax.experimental.pallas import tpu as pltpu
from jax.sharding import PartitionSpec as P


HEAD_SIZE = 64


EPS = 1e-05


def rms_norm(stream, gain):
    mean_sq = jnp.mean(stream * stream, axis=-1, keepdims=True)
    return (stream * lax.rsqrt(mean_sq + EPS) * gain).astype(jnp.bfloat16)


def attention_kernel(
    sinks_ref, len_ref, pre_q_ref, pre_kv_ref, dec_q_ref, dec_kv_ref, cache_ref, out_ref
):
    attend(sinks_ref, len_ref, pre_q_ref, pre_kv_ref, dec_q_ref, dec_kv_ref, cache_ref, out_ref)


def start_kernel(
    where_ref,
    sinks_ref,
    len_ref,
    pre_q_ref,
    pre_kv_ref,
    dec_q_ref,
    dec_kv_ref,
    cache_ref,
    pre_x_ref,
    dec_x_ref,
    ids_ref,
    logits_ref,
    out_ref,
    *rest,
    experts,
):
    pieces, x_ref = rest[:-1], rest[-1]
    attend(sinks_ref, len_ref, pre_q_ref, pre_kv_ref, dec_q_ref, dec_kv_ref, cache_ref, out_ref)
    line, core = where_ref[0], where_ref[1]
    half, width = x_ref.shape
    pre_rows = pre_x_ref.shape[0]
    second = jnp.concatenate(
        [pre_x_ref[half:pre_rows].astype(jnp.float32), dec_x_ref[...].astype(jnp.float32)], 0
    )
    x_ref[...] = jnp.where(core == 0, pre_x_ref[:half].astype(jnp.float32), second)
    topk, tokens = ids_ref.shape
    logits = [logits_ref[pl.ds(k, 1), :] for k in range(topk)]
    top = functools.reduce(jnp.maximum, logits)
    expo = [jnp.exp(value - top) for value in logits]
    total = functools.reduce(lambda a, b: a + b, expo)
    tail_width = pieces[0].shape[1] - width // len(pieces)
    place = lax.broadcasted_iota(jnp.int32, (tail_width, tokens), 0)
    factor = jnp.zeros((tail_width, tokens), jnp.float32)
    for k in range(topk):
        factor = factor + jnp.where(place % experts == ids_ref[pl.ds(k, 1), :], expo[k] / total, 0.0)
    high = factor.astype(jnp.bfloat16).astype(jnp.float32)
    factor = jnp.where(place < experts, high, jnp.where(place < 2 * experts, factor - high, 0.0))
    factor = factor.T
    tail = jnp.where(core == 0, factor[:half], factor[half:]).astype(jnp.bfloat16)
    share = width // len(pieces)
    for k, piece in enumerate(pieces):
        begin = pl.multiple_of(lax.rem(line + k, len(pieces)) * share, 128)
        piece[:, :share] = x_ref[:, pl.ds(begin, share)].astype(jnp.bfloat16)
        piece[:, share:] = tail


def attend(sinks_ref, len_ref, pre_q_ref, pre_kv_ref, dec_q_ref, dec_kv_ref, cache_ref, out_ref):
    pre_rows, q_width = pre_q_ref.shape
    dec_rows = dec_q_ref.shape[0]
    lanes = 2 * HEAD_SIZE
    group = (q_width // HEAD_SIZE) // (pre_kv_ref.shape[2] // HEAD_SIZE)
    scale = HEAD_SIZE ** (-0.5)
    padded = -(-pre_rows // 16) * 16
    positions = cache_ref.shape[2]

    def lane(rows):
        return lax.broadcasted_iota(jnp.int32, (rows, lanes), 1)

    def aligned(pair, side, head, rows):
        value = pair if side == head % 2 else pltpu.roll(pair, HEAD_SIZE, 1)
        return jnp.where((lane(rows) // HEAD_SIZE) == head % 2, value, 0.0)

    def joined(low, high, head, rows):
        low = low if head % 2 == 0 else pltpu.roll(low, HEAD_SIZE, 1)
        high = high if head % 2 == 1 else pltpu.roll(high, HEAD_SIZE, 1)
        return jnp.where(lane(rows) < HEAD_SIZE, low, high)

    def weights(scores, sink, more=None):
        top = jnp.maximum(jnp.max(scores, axis=-1, keepdims=True), sink)
        if more is not None:
            top = jnp.maximum(top, more)
        expo = jnp.exp(scores - top)
        total = jnp.sum(expo, axis=-1, keepdims=True) + jnp.exp(sink - top)
        if more is None:
            return (expo / total).astype(jnp.bfloat16), None
        extra = jnp.exp(more - top)
        total = total + extra
        return (expo / total).astype(jnp.bfloat16), (extra / total).astype(jnp.bfloat16)

    def filled(value):
        return jnp.concatenate(
            [value.astype(jnp.float32), jnp.zeros((padded - pre_rows, lanes), jnp.float32)], 0
        ).astype(jnp.bfloat16)

    contract = (((1,), (1,)), ((), ()))
    key_at = lax.broadcasted_iota(jnp.int32, (pre_rows, padded), 1)
    visible = key_at <= lax.broadcasted_iota(jnp.int32, (pre_rows, padded), 0)
    row_seq = lax.broadcasted_iota(jnp.int32, (dec_rows, positions), 0)
    length = jnp.zeros((dec_rows, positions), jnp.int32)
    for s in range(dec_rows):
        length = jnp.where(row_seq == s, len_ref[s], length)
    live = lax.broadcasted_iota(jnp.int32, (dec_rows, positions), 1) < length

    for head in range(pre_kv_ref.shape[2] // HEAD_SIZE):
        at_lanes = pl.ds((head // 2) * lanes, lanes)
        first_pair = head * group // 2
        here = range(first_pair, first_pair + group // 2)
        stacked = []
        for p in here:
            pair = pre_q_ref[:, pl.ds(p * lanes, lanes)].astype(jnp.float32)
            stacked += [aligned(pair, side, head, pre_rows) for side in (0, 1)]
        queries = jnp.concatenate(stacked, axis=0).astype(jnp.bfloat16)
        keys = filled(pre_kv_ref[0, :, at_lanes])
        scores = lax.dot_general(queries, keys, contract, preferred_element_type=jnp.float32)
        probs = []
        for i in range(group):
            block = scores[i * pre_rows : (i + 1) * pre_rows] * scale
            block = jnp.where(visible, block, -jnp.inf)
            probs.append(weights(block, sinks_ref[head * group + i])[0].astype(jnp.float32))
        pre_out = jnp.dot(
            jnp.concatenate(probs, axis=0).astype(jnp.bfloat16),
            filled(pre_kv_ref[1, :, at_lanes]),
            preferred_element_type=jnp.float32,
        )
        stacked = []
        for p in here:
            pair = dec_q_ref[:, pl.ds(p * lanes, lanes)].astype(jnp.float32)
            stacked += [aligned(pair, side, head, dec_rows) for side in (0, 1)]
        flat = jnp.concatenate(stacked, axis=0)
        queries = flat.astype(jnp.bfloat16)
        owner = lax.broadcasted_iota(jnp.int32, (group * dec_rows, positions), 0) % dec_rows
        past = jnp.zeros((group * dec_rows, positions), jnp.float32)
        for s in range(dec_rows):
            block = lax.dot_general(
                queries, cache_ref[0, s, :, at_lanes], contract, preferred_element_type=jnp.float32
            )
            past = jnp.where(owner == s, block, past)
        own_keys = dec_kv_ref[0, :, at_lanes].astype(jnp.float32)
        own_values = dec_kv_ref[1, :, at_lanes].astype(jnp.float32)
        probs, extras = [], []
        for i in range(group):
            rows = slice(i * dec_rows, (i + 1) * dec_rows)
            block = jnp.where(live, past[rows] * scale, -jnp.inf)
            own = jnp.sum(flat[rows] * own_keys, axis=1, keepdims=True) * scale
            prob, extra = weights(block, sinks_ref[head * group + i], own)
            probs.append(prob.astype(jnp.float32))
            extras.append(extra.astype(jnp.float32) * own_values)
        probs = jnp.concatenate(probs, axis=0)
        dec_out = jnp.concatenate(extras, axis=0)
        for s in range(dec_rows):
            dec_out = dec_out + jnp.dot(
                jnp.where(owner == s, probs, 0.0).astype(jnp.bfloat16),
                cache_ref[1, s, :, at_lanes],
                preferred_element_type=jnp.float32,
            )
        for n, p in enumerate(here):
            low, high = 2 * n, 2 * n + 1
            pre_pair = joined(
                pre_out[low * pre_rows : (low + 1) * pre_rows],
                pre_out[high * pre_rows : (high + 1) * pre_rows],
                head,
                pre_rows,
            )
            dec_pair = joined(
                dec_out[low * dec_rows : (low + 1) * dec_rows],
                dec_out[high * dec_rows : (high + 1) * dec_rows],
                head,
                dec_rows,
            )
            out_ref[:, pl.ds(p * lanes, lanes)] = jnp.concatenate([pre_pair, dec_pair], 0).astype(
                out_ref.dtype
            )


def attention(
    prefill_query_rows,
    prefill_key_values,
    decode_query_rows,
    decode_key_values,
    cache,
    cache_len,
    sinks,
):
    rows = prefill_query_rows.shape[0] + decode_query_rows.shape[0]
    width = prefill_query_rows.shape[1]
    scalars = pl.BlockSpec(memory_space=pltpu.SMEM)
    vectors = pl.BlockSpec(memory_space=pltpu.VMEM)
    return pl.pallas_call(
        attention_kernel,
        out_shape=jax.ShapeDtypeStruct((rows, width), jnp.bfloat16),
        in_specs=[scalars] * 2 + [vectors] * 5,
        out_specs=vectors,
        cost_estimate=pl.CostEstimate(
            flops=4_000_000_000, bytes_accessed=1_000_000, transcendentals=200_000
        ),
        compiler_params=pltpu.CompilerParams(vmem_limit_bytes=8 * 2**20),
        name="attention",
    )(
        sinks,
        cache_len,
        prefill_query_rows,
        prefill_key_values,
        decode_query_rows,
        decode_key_values,
        cache,
    )


def from_hbm(*values):
    return [pltpu.with_memory_space_constraint(v, pltpu.HBM) for v in values]


SCALARS = pl.BlockSpec(memory_space=pltpu.SMEM)
VECTORS = pl.BlockSpec(memory_space=pltpu.VMEM)


def start(where, inputs, x_pre, x_dec, expert_ids, route_logits, experts, deep):
    queries = inputs[0]
    rows = x_pre.shape[0] + x_dec.shape[0]
    half, width = rows // 2, x_pre.shape[1]
    piece = jax.ShapeDtypeStruct(
        (half, width // deep + -(-2 * experts // 128) * 128), jnp.bfloat16
    )
    pre_q, pre_kv, dec_q, dec_kv, cache, cache_len, sinks = inputs
    outs = pl.pallas_call(
        functools.partial(start_kernel, experts=experts),
        out_shape=[jax.ShapeDtypeStruct((rows, queries.shape[1]), jnp.bfloat16)] + [piece] * deep,
        in_specs=[SCALARS] * 3 + [VECTORS] * 9,
        out_specs=[VECTORS] * (deep + 1),
        scratch_shapes=[pltpu.VMEM((half, width), jnp.float32)],
        cost_estimate=pl.CostEstimate(
            flops=4_000_000_000, bytes_accessed=1_000_000, transcendentals=200_000
        ),
        compiler_params=pltpu.CompilerParams(vmem_limit_bytes=8 * 2**20),
        name="start",
    )(
        where,
        *from_hbm(sinks, cache_len, pre_q, pre_kv, dec_q, dec_kv, cache, x_pre, x_dec),
        *from_hbm(expert_ids.T, route_logits.T),
    )
    return outs[0], outs[1:]


def project_kernel(where_ref, *refs, deep):
    attn = refs[:deep]
    columns, beside, across = refs[deep : deep + 3]
    pieces = refs[deep + 3 : 2 * deep + 3]
    kept_ref, given_ref, tail_ref, weight_ref = refs[2 * deep + 3 :]
    line, core, spot = where_ref[0], where_ref[1], where_ref[2]
    count = columns.shape[0]
    for near in range(PLANE):
        other = (near >> 1) | ((near & 1) << 1)
        chip = jnp.bitwise_xor(spot, jnp.where(core == 0, near, other))
        block = (columns, beside, across.at[0], across.at[1])[near]
        weight_ref[pl.ds(pl.multiple_of(chip * count, 16), count), :] = block[...]
    half, share = kept_ref.shape[1], kept_ref.shape[2]
    for k in range(deep):
        part = lax.dot_general(
            attn[k][...],
            weight_ref[...],
            (((1,), (1,)), ((), ())),
            preferred_element_type=jnp.float32,
        )
        chip = lax.rem(line + deep - k, deep)
        mine = jnp.where(core == 0, part[:half], part[half:])
        kept_ref[chip] = mine + pieces[k][:, :share].astype(jnp.float32)
        given_ref[chip] = jnp.where(core == 0, part[half:], part[:half])
        tail_ref[chip] = pieces[k][:, share:]


def project(where, attn, columns, beside, across, pieces):
    deep, half = len(attn), pieces[0].shape[0]
    share = PLANE * columns.shape[0]
    tail = pieces[0].shape[1] - share
    blocks = jax.ShapeDtypeStruct((deep, half, share), jnp.float32)
    return pl.pallas_call(
        functools.partial(project_kernel, deep=deep),
        out_shape=[blocks, blocks, jax.ShapeDtypeStruct((deep, half, tail), jnp.bfloat16)],
        in_specs=[SCALARS] + [VECTORS] * (2 * deep + 3),
        out_specs=[VECTORS] * 3,
        scratch_shapes=[pltpu.VMEM((share, columns.shape[1]), jnp.bfloat16)],
        cost_estimate=pl.CostEstimate(
            flops=4 * deep * half * share * columns.shape[1],
            bytes_accessed=2_000_000,
            transcendentals=0,
        ),
        compiler_params=pltpu.CompilerParams(vmem_limit_bytes=8 * 2**20),
        name="project",
    )(where, *attn, columns, beside, across, *pieces)


def norm_kernel(where_ref, gain_ref, tail_ref, *refs):
    blocks = refs[:-3]
    tokens_ref, own_ref, stream_ref = refs[-3:]
    deep, line = len(blocks), where_ref[0]
    chips, half, share = blocks[0].shape
    for k, block in enumerate(blocks):
        begin = pl.multiple_of(lax.rem(line + deep - k, deep) * share, 128)
        stream_ref[:, pl.ds(begin, share)] = (
            block[...].astype(jnp.float32).reshape(chips * half, share)
        )
    width = deep * share
    stream = stream_ref[...]
    mean_sq = jnp.sum(stream * stream, axis=-1, keepdims=True) * (1.0 / width)
    tokens_ref[:, :width] = (stream * lax.rsqrt(mean_sq + EPS) * gain_ref[...]).astype(jnp.bfloat16)
    tokens_ref[:, width:] = tail_ref[...].reshape(chips * half, tail_ref.shape[2])
    own_ref[...] = stream_ref[pl.ds(pl.multiple_of(line * half, 8), half), :]


def norm(where, gain, tails, blocks):
    chips, half, share = blocks[0].shape
    width = len(blocks) * share
    return pl.pallas_call(
        norm_kernel,
        out_shape=[
            jax.ShapeDtypeStruct((chips * half, width + tails.shape[2]), jnp.bfloat16),
            jax.ShapeDtypeStruct((half, width), jnp.float32),
        ],
        in_specs=[SCALARS] + [VECTORS] * (2 + len(blocks)),
        out_specs=[VECTORS] * 2,
        scratch_shapes=[pltpu.VMEM((chips * half, width), jnp.float32)],
        cost_estimate=pl.CostEstimate(
            flops=1_000_000_000, bytes_accessed=1_000_000, transcendentals=1000
        ),
        compiler_params=pltpu.CompilerParams(vmem_limit_bytes=8 * 2**20),
        name="norm",
    )(where, gain.reshape(1, width), tails, *blocks)


def slot_count(tokens_here, topk, experts):
    return min(
        tokens_here, 2 * ((3 * max(1, (tokens_here * topk + experts - 1) // experts) + 3) // 4)
    )


def slot_plan(
    attn_rows, resid, o_weight, norm_gain, expert_ids, route_logits, w_gate_up, w_down
):
    width = resid.shape[1]
    half = attn_rows.shape[0] // 2
    mine = lax.axis_index("hp") * half
    head_part = jnp.dot(
        attn_rows,
        lax.all_gather(o_weight, "ep", axis=1, tiled=True),
        preferred_element_type=jnp.float32,
    )
    summed = lax.psum_scatter(head_part, "hp", scatter_dimension=0, tiled=True)
    stream = lax.dynamic_slice_in_dim(resid, mine, half, 0).astype(jnp.float32) + summed
    normed = lax.all_gather(rms_norm(stream, norm_gain), "hp", axis=0, tiled=True)
    tokens_here, topk = expert_ids.shape
    holders = lax.axis_size("ep")
    experts = holders // 2
    slot = slot_count(tokens_here, topk, experts)
    plane = slot // 2
    flat_ids = expert_ids.reshape(-1)
    onehot = (flat_ids[:, None] == jnp.arange(experts, dtype=jnp.int32)[None, :]).astype(jnp.int32)
    rank = jnp.sum(jnp.cumsum(onehot, axis=0) * onehot, axis=1) - 1
    position = (flat_ids * slot + rank).reshape(tokens_here, topk)
    columns = jnp.arange(experts * slot, dtype=jnp.int32)[None, None, :] == position[:, :, None]
    picked_rows = jnp.any(columns, axis=1).T.astype(jnp.bfloat16)
    per_expert = (
        jnp.dot(picked_rows, normed, preferred_element_type=jnp.float32)
        .astype(jnp.bfloat16)
        .reshape(experts, slot, width)
    )
    send = jnp.repeat(per_expert, 2, axis=0)
    own_plane = lax.dynamic_slice_in_dim(send, lax.axis_index("hp") * plane, plane, 1)
    arrived_plane = lax.all_to_all(own_plane, "ep", split_axis=0, concat_axis=0, tiled=True)
    arrived = lax.all_gather(arrived_plane, "hp", axis=1, tiled=True)
    rows = arrived.reshape(-1, width)
    gate = jnp.dot(rows, w_gate_up[0, 0], preferred_element_type=jnp.float32)
    upper = jnp.dot(rows, w_gate_up[0, 1], preferred_element_type=jnp.float32)
    hidden = ((upper + 1.0) * gate * jax.nn.sigmoid(1.702 * gate)).astype(jnp.bfloat16)
    partial_out = jnp.dot(hidden, w_down[0], preferred_element_type=jnp.float32).reshape(
        -1, slot, width
    )
    share = lax.psum_scatter(
        partial_out.astype(jnp.bfloat16), "hp", scatter_dimension=1, tiled=True
    )
    returned = lax.all_to_all(share, "ep", split_axis=0, concat_axis=0, tiled=True)
    mix = jax.nn.softmax(route_logits, axis=-1)
    blend = jnp.sum(jnp.where(columns, mix[:, :, None], 0.0), axis=1).reshape(
        tokens_here, experts, slot
    )
    blend = jnp.repeat(blend, 2, axis=1)
    blend_plane = lax.dynamic_slice_in_dim(blend, lax.axis_index("hp") * plane, plane, 2).reshape(
        tokens_here, holders * plane
    )
    terms = jnp.dot(
        blend_plane,
        returned.reshape(-1, width).astype(jnp.float32),
        precision=lax.Precision.HIGHEST,
    )
    moe = lax.psum_scatter(
        terms.astype(jnp.bfloat16), "hp", scatter_dimension=0, tiled=True
    ).astype(jnp.float32)
    return (stream + moe).astype(jnp.bfloat16)


def expert_kernel(mine_ref, rows_ref, gate_up_a, gate_up_b, down_a, down_b, out_ref, *, experts):
    width = gate_up_a.shape[1]
    inputs = rows_ref[:, :width]
    tail = rows_ref[:, width:].astype(jnp.float32)
    lanes = lax.broadcasted_iota(jnp.int32, tail.shape, 1)
    mine = mine_ref[0]
    scale = jnp.sum(
        jnp.where((lanes == mine) | (lanes == mine + experts), tail, 0.0), 1, keepdims=True
    )
    total = None
    for gate_up, down in ((gate_up_a, down_a), (gate_up_b, down_b)):
        gate = jnp.dot(inputs, gate_up[0], preferred_element_type=jnp.float32)
        upper = jnp.dot(inputs, gate_up[1], preferred_element_type=jnp.float32)
        hidden = ((upper + 1.0) * gate * jax.nn.sigmoid(1.702 * gate)).astype(jnp.bfloat16)
        part = jnp.dot(hidden, down[...], preferred_element_type=jnp.float32)
        total = part if total is None else total + part
    out_ref[...] = (total * scale).astype(out_ref.dtype)


def expert_rows(mine, rows, weights, experts, out_type):
    count, width, units = rows.shape[0], weights[0].shape[1], 2 * weights[0].shape[2]
    vectors = pl.BlockSpec(memory_space=pltpu.VMEM)
    return pl.pallas_call(
        functools.partial(expert_kernel, experts=experts),
        out_shape=jax.ShapeDtypeStruct((count, width), out_type),
        in_specs=[pl.BlockSpec(memory_space=pltpu.SMEM)] + [vectors] * 5,
        out_specs=vectors,
        cost_estimate=pl.CostEstimate(
            flops=6 * count * width * units,
            bytes_accessed=6 * width * units,
            transcendentals=count * units,
        ),
        compiler_params=pltpu.CompilerParams(vmem_limit_bytes=12 * 2**20),
        name="expert",
    )(mine, rows, *weights)


PLANE = 4


def plane_perm(holders, stage):
    return [
        (2 * e + h, 2 * (e ^ (1 if h == stage else 2)) + h) for e in range(holders) for h in (0, 1)
    ]


def line_perm(holders, step):
    return [(e, (e + PLANE * step) % holders) for e in range(holders)]


def at(blocks, index):
    return lax.dynamic_index_in_dim(blocks, index, 0, keepdims=False)


def dense_plan(
    inputs, x_pre, x_dec, o_weight, norm_gain, expert_ids, route_logits, w_gate_up, w_down
):
    tokens_here, width = x_pre.shape[0] + x_dec.shape[0], x_pre.shape[1]
    holders = lax.axis_size("ep")
    experts = holders // 2
    deep = holders // PLANE
    place, core = lax.axis_index("ep"), lax.axis_index("hp")
    line, spot = place // PLANE, place % PLANE
    half = tokens_here // 2
    swap = [(0, 1), (1, 0)]
    far_first = range(deep - 1, 0, -1)
    where = jnp.stack([line, core, spot]).astype(jnp.int32)

    def plane(value, stage):
        return lax.ppermute(value, ("ep", "hp"), plane_perm(holders, stage))

    def along(value, step):
        return lax.ppermute(value, "ep", line_perm(holders, step))

    def gather_line(value):
        got = {k: along(value, k) for k in far_first}
        return [value] + [got[k] for k in range(1, deep)]

    gate_up_here, down_here = w_gate_up[0], w_down[0]
    gate_up_there = lax.ppermute(gate_up_here, "hp", swap)
    down_there = lax.ppermute(down_here, "hp", swap)

    columns = o_weight.T
    beside = plane(columns, 0)
    across = plane(jnp.stack([columns, beside]), 1)

    attn_rows, pieces = start(where, inputs, x_pre, x_dec, expert_ids, route_logits, experts, deep)
    attn = gather_line(attn_rows)
    arrived = {k: along(pieces[k], k) for k in far_first}
    arrived[0] = pieces[0]
    kept, given, tails = project(
        where, attn, columns, beside, across, [arrived[k] for k in range(deep)]
    )
    given, gate_up_there, down_there = lax.optimization_barrier((given, gate_up_there, down_there))
    weights = tuple(
        pltpu.with_memory_space_constraint(w, pltpu.VMEM)
        for w in (gate_up_here, gate_up_there, down_here, down_there)
    )
    summed = (kept + lax.ppermute(given, "hp", swap)).astype(jnp.bfloat16)
    tokens, own_stream = norm(where, norm_gain, tails, gather_line(summed))

    mine = jnp.reshape(place // 2, (1,))

    def expert(block, out_type):
        return expert_rows(mine, block, weights, experts, out_type)

    near_tokens = plane(tokens, 0)
    both_tokens = plane(near_tokens, 1)
    far_tokens = plane(tokens, 1)
    own = expert(tokens, jnp.float32)
    near_out = expert(near_tokens, jnp.bfloat16)
    both_out = expert(both_tokens, jnp.bfloat16)
    far_out = expert(far_tokens, jnp.float32)
    far_back = plane(both_out, 0)
    near_back = plane(near_out, 0)
    over = plane((far_out + far_back.astype(jnp.float32)).astype(jnp.bfloat16), 1)
    moe = own + near_back.astype(jnp.float32) + over.astype(jnp.float32)
    moe = moe.reshape(deep, half, width)
    sent = moe.astype(jnp.bfloat16)
    got = [along(at(sent, (line + k) % deep), k) for k in far_first]
    total = own_stream + at(moe, line)
    for block in got:
        total = total + block.astype(jnp.float32)
    return total.astype(jnp.bfloat16)


def on_device(
    x_pre,
    x_dec,
    prefill_query_rows,
    prefill_key_values,
    decode_query_rows,
    decode_key_values,
    cache,
    cache_len,
    sinks,
    o_weight,
    norm_gain,
    expert_ids,
    route_logits,
    w_gate_up,
    w_down,
):
    inputs = (
        prefill_query_rows,
        prefill_key_values,
        decode_query_rows,
        decode_key_values,
        cache,
        cache_len,
        sinks,
    )
    rest = (o_weight, norm_gain, expert_ids, route_logits, w_gate_up, w_down)
    tokens_here, topk = expert_ids.shape
    holders = lax.axis_size("ep")
    dense = tokens_here <= 2 * slot_count(tokens_here, topk, holders // 2)
    even = holders % PLANE == 0 and x_pre.shape[1] % (holders // PLANE * 128) == 0
    if dense and even and holders > PLANE and lax.axis_size("hp") == 2:
        return dense_plan(inputs, x_pre, x_dec, *rest)
    return slot_plan(attention(*inputs), jnp.concatenate([x_pre, x_dec], axis=0), *rest)


def solution(mesh):
    placed = (
        P(("groups", "ep"), None),
        P(("groups", "ep"), None),
        P(("groups", "ep"), "hp"),
        P(None, ("groups", "ep"), "hp"),
        P(("groups", "ep"), "hp"),
        P(None, ("groups", "ep"), "hp"),
        P(None, ("groups", "ep"), None, "hp"),
        P(("groups", "ep")),
        P("hp"),
        P("hp", "ep"),
        P(),
        P(("groups", "ep"), None),
        P(("groups", "ep"), None),
        P("ep", None, None, "hp"),
        P("ep", "hp", None),
    )
    return jax.shard_map(
        on_device,
        mesh=mesh,
        in_specs=placed,
        out_specs=P(("groups", "ep", "hp"), None),
        check_vma=False,
    )
```

```python
import functools
import jax
import jax.numpy as jnp
from jax import lax
from jax.experimental import pallas as pl
from jax.experimental.pallas import tpu as pltpu
from jax.sharding import PartitionSpec as P


HEAD_SIZE = 64


EPS = 1e-05


def rms_norm(stream, gain):
    mean_sq = jnp.mean(stream * stream, axis=-1, keepdims=True)
    return (stream * lax.rsqrt(mean_sq + EPS) * gain).astype(jnp.bfloat16)


def attention_kernel(
    sinks_ref, len_ref, pre_q_ref, pre_kv_ref, dec_q_ref, dec_kv_ref, cache_ref, out_ref
):
    attend(sinks_ref, len_ref, pre_q_ref, pre_kv_ref, dec_q_ref, dec_kv_ref, cache_ref, out_ref)


def start_kernel(
    line_ref,
    core_ref,
    spot_ref,
    mine_ref,
    sinks_ref,
    len_ref,
    pre_q_ref,
    pre_kv_ref,
    dec_q_ref,
    dec_kv_ref,
    cache_ref,
    pre_x_ref,
    dec_x_ref,
    ids_ref,
    logits_ref,
    out_ref,
    *rest,
    experts,
):
    pieces, x_ref = rest[:-1], rest[-1]
    attend(sinks_ref, len_ref, pre_q_ref, pre_kv_ref, dec_q_ref, dec_kv_ref, cache_ref, out_ref)
    line, core = line_ref[0], core_ref[0]
    half, width = x_ref.shape
    pre_rows = pre_x_ref.shape[0]
    second = jnp.concatenate(
        [pre_x_ref[half:pre_rows].astype(jnp.float32), dec_x_ref[...].astype(jnp.float32)], 0
    )
    x_ref[...] = jnp.where(core == 0, pre_x_ref[:half].astype(jnp.float32), second)
    topk, tokens = ids_ref.shape
    logits = [logits_ref[pl.ds(k, 1), :] for k in range(topk)]
    top = functools.reduce(jnp.maximum, logits)
    expo = [jnp.exp(value - top) for value in logits]
    total = functools.reduce(lambda a, b: a + b, expo)
    tail_width = pieces[0].shape[1] - width // len(pieces)
    place = lax.broadcasted_iota(jnp.int32, (tail_width, tokens), 0)
    factor = jnp.zeros((tail_width, tokens), jnp.float32)
    for k in range(topk):
        factor = factor + jnp.where(place % experts == ids_ref[pl.ds(k, 1), :], expo[k] / total, 0.0)
    high = factor.astype(jnp.bfloat16).astype(jnp.float32)
    factor = jnp.where(place < experts, high, jnp.where(place < 2 * experts, factor - high, 0.0))
    factor = factor.T
    tail = jnp.where(core == 0, factor[:half], factor[half:]).astype(jnp.bfloat16)
    share = width // len(pieces)
    for k, piece in enumerate(pieces):
        begin = pl.multiple_of(lax.rem(line + k, len(pieces)) * share, 128)
        piece[:, :share] = x_ref[:, pl.ds(begin, share)].astype(jnp.bfloat16)
        piece[:, share:] = tail


def attend(sinks_ref, len_ref, pre_q_ref, pre_kv_ref, dec_q_ref, dec_kv_ref, cache_ref, out_ref):
    pre_rows, q_width = pre_q_ref.shape
    dec_rows = dec_q_ref.shape[0]
    lanes = 2 * HEAD_SIZE
    group = (q_width // HEAD_SIZE) // (pre_kv_ref.shape[2] // HEAD_SIZE)
    scale = HEAD_SIZE ** (-0.5)
    padded = -(-pre_rows // 16) * 16
    positions = cache_ref.shape[2]

    def lane(rows):
        return lax.broadcasted_iota(jnp.int32, (rows, lanes), 1)

    def aligned(pair, side, head, rows):
        value = pair if side == head % 2 else pltpu.roll(pair, HEAD_SIZE, 1)
        return jnp.where((lane(rows) // HEAD_SIZE) == head % 2, value, 0.0)

    def joined(low, high, head, rows):
        low = low if head % 2 == 0 else pltpu.roll(low, HEAD_SIZE, 1)
        high = high if head % 2 == 1 else pltpu.roll(high, HEAD_SIZE, 1)
        return jnp.where(lane(rows) < HEAD_SIZE, low, high)

    def weights(scores, sink, more=None):
        top = jnp.maximum(jnp.max(scores, axis=-1, keepdims=True), sink)
        if more is not None:
            top = jnp.maximum(top, more)
        expo = jnp.exp(scores - top)
        total = jnp.sum(expo, axis=-1, keepdims=True) + jnp.exp(sink - top)
        if more is None:
            return (expo / total).astype(jnp.bfloat16), None
        extra = jnp.exp(more - top)
        total = total + extra
        return (expo / total).astype(jnp.bfloat16), (extra / total).astype(jnp.bfloat16)

    def filled(value):
        return jnp.concatenate(
            [value.astype(jnp.float32), jnp.zeros((padded - pre_rows, lanes), jnp.float32)], 0
        ).astype(jnp.bfloat16)

    contract = (((1,), (1,)), ((), ()))
    key_at = lax.broadcasted_iota(jnp.int32, (pre_rows, padded), 1)
    visible = key_at <= lax.broadcasted_iota(jnp.int32, (pre_rows, padded), 0)
    row_seq = lax.broadcasted_iota(jnp.int32, (dec_rows, positions), 0)
    length = jnp.zeros((dec_rows, positions), jnp.int32)
    for s in range(dec_rows):
        length = jnp.where(row_seq == s, len_ref[s], length)
    live = lax.broadcasted_iota(jnp.int32, (dec_rows, positions), 1) < length

    for head in range(pre_kv_ref.shape[2] // HEAD_SIZE):
        at_lanes = pl.ds((head // 2) * lanes, lanes)
        first_pair = head * group // 2
        here = range(first_pair, first_pair + group // 2)
        stacked = []
        for p in here:
            pair = pre_q_ref[:, pl.ds(p * lanes, lanes)].astype(jnp.float32)
            stacked += [aligned(pair, side, head, pre_rows) for side in (0, 1)]
        queries = jnp.concatenate(stacked, axis=0).astype(jnp.bfloat16)
        keys = filled(pre_kv_ref[0, :, at_lanes])
        scores = lax.dot_general(queries, keys, contract, preferred_element_type=jnp.float32)
        probs = []
        for i in range(group):
            block = scores[i * pre_rows : (i + 1) * pre_rows] * scale
            block = jnp.where(visible, block, -jnp.inf)
            probs.append(weights(block, sinks_ref[head * group + i])[0].astype(jnp.float32))
        pre_out = jnp.dot(
            jnp.concatenate(probs, axis=0).astype(jnp.bfloat16),
            filled(pre_kv_ref[1, :, at_lanes]),
            preferred_element_type=jnp.float32,
        )
        stacked = []
        for p in here:
            pair = dec_q_ref[:, pl.ds(p * lanes, lanes)].astype(jnp.float32)
            stacked += [aligned(pair, side, head, dec_rows) for side in (0, 1)]
        flat = jnp.concatenate(stacked, axis=0)
        queries = flat.astype(jnp.bfloat16)
        owner = lax.broadcasted_iota(jnp.int32, (group * dec_rows, positions), 0) % dec_rows
        past = jnp.zeros((group * dec_rows, positions), jnp.float32)
        for s in range(dec_rows):
            block = lax.dot_general(
                queries, cache_ref[0, s, :, at_lanes], contract, preferred_element_type=jnp.float32
            )
            past = jnp.where(owner == s, block, past)
        own_keys = dec_kv_ref[0, :, at_lanes].astype(jnp.float32)
        own_values = dec_kv_ref[1, :, at_lanes].astype(jnp.float32)
        probs, extras = [], []
        for i in range(group):
            rows = slice(i * dec_rows, (i + 1) * dec_rows)
            block = jnp.where(live, past[rows] * scale, -jnp.inf)
            own = jnp.sum(flat[rows] * own_keys, axis=1, keepdims=True) * scale
            prob, extra = weights(block, sinks_ref[head * group + i], own)
            probs.append(prob.astype(jnp.float32))
            extras.append(extra.astype(jnp.float32) * own_values)
        probs = jnp.concatenate(probs, axis=0)
        dec_out = jnp.concatenate(extras, axis=0)
        for s in range(dec_rows):
            dec_out = dec_out + jnp.dot(
                jnp.where(owner == s, probs, 0.0).astype(jnp.bfloat16),
                cache_ref[1, s, :, at_lanes],
                preferred_element_type=jnp.float32,
            )
        for n, p in enumerate(here):
            low, high = 2 * n, 2 * n + 1
            pre_pair = joined(
                pre_out[low * pre_rows : (low + 1) * pre_rows],
                pre_out[high * pre_rows : (high + 1) * pre_rows],
                head,
                pre_rows,
            )
            dec_pair = joined(
                dec_out[low * dec_rows : (low + 1) * dec_rows],
                dec_out[high * dec_rows : (high + 1) * dec_rows],
                head,
                dec_rows,
            )
            out_ref[:, pl.ds(p * lanes, lanes)] = jnp.concatenate([pre_pair, dec_pair], 0).astype(
                out_ref.dtype
            )


def attention(
    prefill_query_rows,
    prefill_key_values,
    decode_query_rows,
    decode_key_values,
    cache,
    cache_len,
    sinks,
):
    rows = prefill_query_rows.shape[0] + decode_query_rows.shape[0]
    width = prefill_query_rows.shape[1]
    scalars = pl.BlockSpec(memory_space=pltpu.SMEM)
    vectors = pl.BlockSpec(memory_space=pltpu.VMEM)
    return pl.pallas_call(
        attention_kernel,
        out_shape=jax.ShapeDtypeStruct((rows, width), jnp.bfloat16),
        in_specs=[scalars] * 2 + [vectors] * 5,
        out_specs=vectors,
        cost_estimate=pl.CostEstimate(
            flops=4_000_000_000, bytes_accessed=1_000_000, transcendentals=200_000
        ),
        compiler_params=pltpu.CompilerParams(vmem_limit_bytes=8 * 2**20),
        name="attention",
    )(
        sinks,
        cache_len,
        prefill_query_rows,
        prefill_key_values,
        decode_query_rows,
        decode_key_values,
        cache,
    )


def from_hbm(*values):
    return [pltpu.with_memory_space_constraint(v, pltpu.HBM) for v in values]


SCALARS = pl.BlockSpec(memory_space=pltpu.SMEM)
VECTORS = pl.BlockSpec(memory_space=pltpu.VMEM)


def start(where, inputs, x_pre, x_dec, expert_ids, route_logits, experts, deep):
    queries = inputs[0]
    rows = x_pre.shape[0] + x_dec.shape[0]
    half, width = rows // 2, x_pre.shape[1]
    piece = jax.ShapeDtypeStruct(
        (half, width // deep + -(-2 * experts // 128) * 128), jnp.bfloat16
    )
    pre_q, pre_kv, dec_q, dec_kv, cache, cache_len, sinks = inputs
    outs = pl.pallas_call(
        functools.partial(start_kernel, experts=experts),
        out_shape=[jax.ShapeDtypeStruct((rows, queries.shape[1]), jnp.bfloat16)] + [piece] * deep,
        in_specs=[SCALARS] * 6 + [VECTORS] * 9,
        out_specs=[VECTORS] * (deep + 1),
        scratch_shapes=[pltpu.VMEM((half, width), jnp.float32)],
        cost_estimate=pl.CostEstimate(
            flops=4_000_000_000, bytes_accessed=1_000_000, transcendentals=200_000
        ),
        compiler_params=pltpu.CompilerParams(vmem_limit_bytes=8 * 2**20),
        name="start",
    )(
        *where,
        *from_hbm(sinks, cache_len, pre_q, pre_kv, dec_q, dec_kv, cache, x_pre, x_dec),
        *from_hbm(expert_ids.T, route_logits.T),
    )
    return outs[0], outs[1:]


def project_kernel(core_ref, spot_ref, *refs, deep):
    attn = refs[:deep]
    columns, beside, across, kept_ref, given_ref, weight_ref = refs[deep:]
    core, spot = core_ref[0], spot_ref[0]
    count = columns.shape[0]
    for near in range(PLANE):
        other = (near >> 1) | ((near & 1) << 1)
        chip = jnp.bitwise_xor(spot, jnp.where(core == 0, near, other))
        block = (columns, beside, across.at[0], across.at[1])[near]
        weight_ref[pl.ds(pl.multiple_of(chip * count, 16), count), :] = block[...]
    half = kept_ref.shape[1]
    parts = lax.dot_general(
        jnp.concatenate([block[...] for block in attn], axis=0),
        weight_ref[...],
        (((1,), (1,)), ((), ())),
        preferred_element_type=jnp.float32,
    )
    for k in range(deep):
        part = parts[2 * half * k : 2 * half * (k + 1)]
        kept_ref[k] = jnp.where(core == 0, part[:half], part[half:])
        given_ref[k] = jnp.where(core == 0, part[half:], part[:half])


def project(core_at, spot_at, attn, columns, beside, across):
    deep, half = len(attn), attn[0].shape[0] // 2
    share = PLANE * columns.shape[0]
    blocks = pltpu.VMEM((deep, half, share), jnp.float32)
    return pl.pallas_call(
        functools.partial(project_kernel, deep=deep),
        out_shape=[blocks, blocks],
        in_specs=[SCALARS] * 2 + [VECTORS] * (deep + 3),
        out_specs=[VECTORS] * 2,
        scratch_shapes=[pltpu.VMEM((share, columns.shape[1]), jnp.bfloat16)],
        cost_estimate=pl.CostEstimate(
            flops=4 * deep * half * share * columns.shape[1],
            bytes_accessed=2_000_000,
            transcendentals=0,
        ),
        compiler_params=pltpu.CompilerParams(vmem_limit_bytes=8 * 2**20),
        name="project",
    )(core_at, spot_at, *attn, columns, beside, across)


def norm_kernel(line_ref, gain_ref, *refs, deep):
    pieces, blocks = refs[:deep], refs[deep : 2 * deep]
    tokens_ref, own_ref = refs[2 * deep :]
    line = line_ref[0]
    _, half, share = blocks[0].shape
    width = deep * share
    order = [[(c - b) % deep for b in range(deep)] for c in range(deep)]
    for c in range(deep):
        values = [blocks[b][order[c][b]].astype(jnp.float32) for b in range(deep)]
        square = functools.reduce(lambda x, y: x + y, [v * v for v in values])
        root = lax.rsqrt(jnp.sum(square, axis=-1, keepdims=True) * (1.0 / width) + EPS)
        rows = pl.ds(pl.multiple_of(lax.rem(line + deep - c, deep) * half, 16), half)
        for b, value in enumerate(values):
            columns = pl.ds(pl.multiple_of(lax.rem(line + deep - b, deep) * share, 128), share)
            tokens_ref[rows, columns] = (value * root * gain_ref[:, columns]).astype(jnp.bfloat16)
            if c == 0:
                own_ref[:, columns] = value
        tokens_ref[rows, width:] = pieces[c][:, share:]


def norm(line_at, gain, pieces, blocks):
    deep, half, share = blocks[0].shape
    width = deep * share
    tail = pieces[0].shape[1] - share
    return pl.pallas_call(
        functools.partial(norm_kernel, deep=deep),
        out_shape=[
            pltpu.VMEM((deep * half, width + tail), jnp.bfloat16),
            pltpu.VMEM((half, width), jnp.float32),
        ],
        in_specs=[SCALARS] + [VECTORS] * (1 + 2 * deep),
        out_specs=[VECTORS] * 2,
        cost_estimate=pl.CostEstimate(
            flops=1_000_000_000, bytes_accessed=1_000_000, transcendentals=1000
        ),
        compiler_params=pltpu.CompilerParams(vmem_limit_bytes=8 * 2**20),
        name="norm",
    )(line_at, gain.reshape(1, width), *pieces, *blocks)


def slot_count(tokens_here, topk, experts):
    return min(
        tokens_here, 2 * ((3 * max(1, (tokens_here * topk + experts - 1) // experts) + 3) // 4)
    )


def slot_plan(
    attn_rows, resid, o_weight, norm_gain, expert_ids, route_logits, w_gate_up, w_down
):
    width = resid.shape[1]
    half = attn_rows.shape[0] // 2
    mine = lax.axis_index("hp") * half
    head_part = jnp.dot(
        attn_rows,
        lax.all_gather(o_weight, "ep", axis=1, tiled=True),
        preferred_element_type=jnp.float32,
    )
    summed = lax.psum_scatter(head_part, "hp", scatter_dimension=0, tiled=True)
    stream = lax.dynamic_slice_in_dim(resid, mine, half, 0).astype(jnp.float32) + summed
    normed = lax.all_gather(rms_norm(stream, norm_gain), "hp", axis=0, tiled=True)
    tokens_here, topk = expert_ids.shape
    holders = lax.axis_size("ep")
    experts = holders // 2
    slot = slot_count(tokens_here, topk, experts)
    plane = slot // 2
    flat_ids = expert_ids.reshape(-1)
    onehot = (flat_ids[:, None] == jnp.arange(experts, dtype=jnp.int32)[None, :]).astype(jnp.int32)
    rank = jnp.sum(jnp.cumsum(onehot, axis=0) * onehot, axis=1) - 1
    position = (flat_ids * slot + rank).reshape(tokens_here, topk)
    columns = jnp.arange(experts * slot, dtype=jnp.int32)[None, None, :] == position[:, :, None]
    picked_rows = jnp.any(columns, axis=1).T.astype(jnp.bfloat16)
    per_expert = (
        jnp.dot(picked_rows, normed, preferred_element_type=jnp.float32)
        .astype(jnp.bfloat16)
        .reshape(experts, slot, width)
    )
    send = jnp.repeat(per_expert, 2, axis=0)
    own_plane = lax.dynamic_slice_in_dim(send, lax.axis_index("hp") * plane, plane, 1)
    arrived_plane = lax.all_to_all(own_plane, "ep", split_axis=0, concat_axis=0, tiled=True)
    arrived = lax.all_gather(arrived_plane, "hp", axis=1, tiled=True)
    rows = arrived.reshape(-1, width)
    gate = jnp.dot(rows, w_gate_up[0, 0], preferred_element_type=jnp.float32)
    upper = jnp.dot(rows, w_gate_up[0, 1], preferred_element_type=jnp.float32)
    hidden = ((upper + 1.0) * gate * jax.nn.sigmoid(1.702 * gate)).astype(jnp.bfloat16)
    partial_out = jnp.dot(hidden, w_down[0], preferred_element_type=jnp.float32).reshape(
        -1, slot, width
    )
    share = lax.psum_scatter(
        partial_out.astype(jnp.bfloat16), "hp", scatter_dimension=1, tiled=True
    )
    returned = lax.all_to_all(share, "ep", split_axis=0, concat_axis=0, tiled=True)
    mix = jax.nn.softmax(route_logits, axis=-1)
    blend = jnp.sum(jnp.where(columns, mix[:, :, None], 0.0), axis=1).reshape(
        tokens_here, experts, slot
    )
    blend = jnp.repeat(blend, 2, axis=1)
    blend_plane = lax.dynamic_slice_in_dim(blend, lax.axis_index("hp") * plane, plane, 2).reshape(
        tokens_here, holders * plane
    )
    terms = jnp.dot(
        blend_plane,
        returned.reshape(-1, width).astype(jnp.float32),
        precision=lax.Precision.HIGHEST,
    )
    moe = lax.psum_scatter(
        terms.astype(jnp.bfloat16), "hp", scatter_dimension=0, tiled=True
    ).astype(jnp.float32)
    return (stream + moe).astype(jnp.bfloat16)


def pack_kernel(gate_up_a, gate_up_b, down_a, down_b, gate_up_ref, down_ref, sems):
    units = down_a.shape[0]
    copies = [
        pltpu.make_async_copy(gate_up_a, gate_up_ref.at[:, :, :units], sems.at[0]),
        pltpu.make_async_copy(gate_up_b, gate_up_ref.at[:, :, units:], sems.at[1]),
        pltpu.make_async_copy(down_a, down_ref.at[:units], sems.at[2]),
        pltpu.make_async_copy(down_b, down_ref.at[units:], sems.at[3]),
    ]
    for copy in copies:
        copy.start()
    for copy in copies:
        copy.wait()


def pack(gate_up_a, gate_up_b, down_a, down_b):
    units, width = down_a.shape
    kinds = gate_up_a.dtype
    return pl.pallas_call(
        pack_kernel,
        out_shape=[pltpu.VMEM((2, width, 2 * units), kinds), pltpu.VMEM((2 * units, width), kinds)],
        in_specs=[pl.BlockSpec(memory_space=pltpu.HBM)] * 4,
        out_specs=[VECTORS] * 2,
        scratch_shapes=[pltpu.SemaphoreType.DMA((4,))],
        cost_estimate=pl.CostEstimate(
            flops=2_000_000_000, bytes_accessed=12 * width * units, transcendentals=0
        ),
        compiler_params=pltpu.CompilerParams(vmem_limit_bytes=10 * 2**20),
        name="pack",
    )(gate_up_a, gate_up_b, down_a, down_b)


def expert_kernel(mine_ref, rows_ref, gate_up, down, out_ref, *, experts):
    width = gate_up.shape[1]
    inputs = rows_ref[:, :width]
    tail = rows_ref[:, width:].astype(jnp.float32)
    lanes = lax.broadcasted_iota(jnp.int32, tail.shape, 1)
    mine = mine_ref[0]
    scale = jnp.sum(
        jnp.where((lanes == mine) | (lanes == mine + experts), tail, 0.0), 1, keepdims=True
    )
    gate = jnp.dot(inputs, gate_up[0], preferred_element_type=jnp.float32)
    upper = jnp.dot(inputs, gate_up[1], preferred_element_type=jnp.float32)
    hidden = ((upper + 1.0) * gate * jax.nn.sigmoid(1.702 * gate)).astype(jnp.bfloat16)
    total = jnp.dot(hidden, down[...], preferred_element_type=jnp.float32)
    out_ref[...] = (total * scale).astype(out_ref.dtype)


def expert_rows(mine_at, rows, weights, experts, out_type):
    count, (units, width) = rows.shape[0], weights[1].shape
    return pl.pallas_call(
        functools.partial(expert_kernel, experts=experts),
        out_shape=pltpu.VMEM((count, width), out_type),
        in_specs=[SCALARS] + [VECTORS] * 3,
        out_specs=VECTORS,
        cost_estimate=pl.CostEstimate(
            flops=6 * count * width * units,
            bytes_accessed=6 * width * units,
            transcendentals=count * units,
        ),
        compiler_params=pltpu.CompilerParams(vmem_limit_bytes=12 * 2**20),
        name="expert",
    )(mine_at, rows, *weights)


def finish_kernel(line_ref, own_ref, near_ref, over_ref, stream_ref, rest_ref, *sent):
    deep, line = len(sent) + 1, line_ref[0]
    half = rest_ref.shape[0]
    for k in range(deep):
        rows = pl.ds(pl.multiple_of(lax.rem(line + k, deep) * half, 16), half)
        total = own_ref[rows, :] + near_ref[rows, :].astype(jnp.float32)
        total = total + over_ref[rows, :].astype(jnp.float32)
        if k == 0:
            rest_ref[...] = stream_ref[...] + total
        else:
            sent[k - 1][...] = total.astype(jnp.bfloat16)


def finish(line_at, own, near_back, over, own_stream, deep):
    half, width = own_stream.shape
    return pl.pallas_call(
        finish_kernel,
        out_shape=[pltpu.VMEM((half, width), jnp.float32)]
        + [pltpu.VMEM((half, width), jnp.bfloat16)] * (deep - 1),
        in_specs=[SCALARS] + [VECTORS] * 4,
        out_specs=[VECTORS] * deep,
        cost_estimate=pl.CostEstimate(
            flops=500_000_000, bytes_accessed=1_000_000, transcendentals=0
        ),
        compiler_params=pltpu.CompilerParams(vmem_limit_bytes=8 * 2**20),
        name="finish",
    )(line_at, own, near_back, over, own_stream)


PLANE = 4


def plane_perm(holders, stage):
    return [
        (2 * e + h, 2 * (e ^ (1 if h == stage else 2)) + h) for e in range(holders) for h in (0, 1)
    ]


def line_perm(holders, step):
    return [(e, (e + PLANE * step) % holders) for e in range(holders)]


def dense_plan(
    inputs, x_pre, x_dec, o_weight, norm_gain, expert_ids, route_logits, w_gate_up, w_down
):
    holders = lax.axis_size("ep")
    experts = holders // 2
    deep = holders // PLANE
    place, core = lax.axis_index("ep"), lax.axis_index("hp")
    line, spot = place // PLANE, place % PLANE
    swap = [(0, 1), (1, 0)]
    far_first = range(deep - 1, 0, -1)
    where = [jnp.reshape(v, (1,)).astype(jnp.int32) for v in (line, core, spot, place // 2)]
    line_at, core_at, spot_at, mine_at = where

    def plane(value, stage):
        return lax.ppermute(value, ("ep", "hp"), plane_perm(holders, stage))

    def along(value, step):
        return lax.ppermute(value, "ep", line_perm(holders, step))

    def gather_line(value):
        got = {k: along(value, k) for k in far_first}
        return [value] + [got[k] for k in range(1, deep)]

    gate_up_here, down_here = w_gate_up[0], w_down[0]
    gate_up_there = lax.ppermute(gate_up_here, "hp", swap)
    down_there = lax.ppermute(down_here, "hp", swap)

    weights = pack(gate_up_here, gate_up_there, down_here, down_there)

    columns = o_weight.T
    beside = plane(columns, 0)
    across = plane(jnp.stack([columns, beside]), 1)

    attn_rows, pieces = start(where, inputs, x_pre, x_dec, expert_ids, route_logits, experts, deep)
    attn = gather_line(attn_rows)
    arrived = {k: along(pieces[k], k) for k in far_first}
    arrived[0] = pieces[0]
    pieces = [arrived[k] for k in range(deep)]
    kept, given = project(core_at, spot_at, attn, columns, beside, across)
    added = jnp.stack([piece[:, : kept.shape[2]] for piece in pieces]).astype(jnp.float32)
    summed = (kept + lax.ppermute(given, "hp", swap) + added).astype(jnp.bfloat16)
    tokens, own_stream = norm(line_at, norm_gain, pieces, gather_line(summed))

    def expert(block, out_type):
        return expert_rows(mine_at, block, weights, experts, out_type)

    near_tokens = plane(tokens, 0)
    both_tokens = plane(near_tokens, 1)
    far_tokens = plane(tokens, 1)
    own = expert(tokens, jnp.float32)
    near_out = expert(near_tokens, jnp.bfloat16)
    both_out = expert(both_tokens, jnp.bfloat16)
    far_out = expert(far_tokens, jnp.float32)
    far_back = plane(both_out, 0)
    near_back = plane(near_out, 0)
    over = plane((far_out + far_back.astype(jnp.float32)).astype(jnp.bfloat16), 1)
    rest, *sent = finish(line_at, own, near_back, over, own_stream, deep)
    got = [along(sent[k - 1], k) for k in far_first]
    for block in got:
        rest = rest + block.astype(jnp.float32)
    return rest.astype(jnp.bfloat16)


def on_device(
    x_pre,
    x_dec,
    prefill_query_rows,
    prefill_key_values,
    decode_query_rows,
    decode_key_values,
    cache,
    cache_len,
    sinks,
    o_weight,
    norm_gain,
    expert_ids,
    route_logits,
    w_gate_up,
    w_down,
):
    inputs = (
        prefill_query_rows,
        prefill_key_values,
        decode_query_rows,
        decode_key_values,
        cache,
        cache_len,
        sinks,
    )
    rest = (o_weight, norm_gain, expert_ids, route_logits, w_gate_up, w_down)
    tokens_here, topk = expert_ids.shape
    holders = lax.axis_size("ep")
    dense = tokens_here <= 2 * slot_count(tokens_here, topk, holders // 2)
    even = holders % PLANE == 0 and x_pre.shape[1] % (holders // PLANE * 128) == 0
    if dense and even and holders > PLANE and lax.axis_size("hp") == 2:
        return dense_plan(inputs, x_pre, x_dec, *rest)
    return slot_plan(attention(*inputs), jnp.concatenate([x_pre, x_dec], axis=0), *rest)


def solution(mesh):
    placed = (
        P(("groups", "ep"), None),
        P(("groups", "ep"), None),
        P(("groups", "ep"), "hp"),
        P(None, ("groups", "ep"), "hp"),
        P(("groups", "ep"), "hp"),
        P(None, ("groups", "ep"), "hp"),
        P(None, ("groups", "ep"), None, "hp"),
        P(("groups", "ep")),
        P("hp"),
        P("hp", "ep"),
        P(),
        P(("groups", "ep"), None),
        P(("groups", "ep"), None),
        P("ep", None, None, "hp"),
        P("ep", "hp", None),
    )
    return jax.shard_map(
        on_device,
        mesh=mesh,
        in_specs=placed,
        out_specs=P(("groups", "ep", "hp"), None),
        check_vma=False,
    )
```

```python
import functools
import jax
import jax.numpy as jnp
from jax import lax
from jax.experimental import pallas as pl
from jax.experimental.pallas import tpu as pltpu
from jax.sharding import PartitionSpec as P


HEAD_SIZE = 64


EPS = 1e-05


def rms_norm(stream, gain):
    mean_sq = jnp.mean(stream * stream, axis=-1, keepdims=True)
    return (stream * lax.rsqrt(mean_sq + EPS) * gain).astype(jnp.bfloat16)


def attention_kernel(
    sinks_ref, len_ref, pre_q_ref, pre_kv_ref, dec_q_ref, dec_kv_ref, cache_ref, out_ref
):
    attend(sinks_ref, len_ref, pre_q_ref, pre_kv_ref, dec_q_ref, dec_kv_ref, cache_ref, out_ref)


def start_kernel(
    line_ref,
    core_ref,
    spot_ref,
    mine_ref,
    sinks_ref,
    len_ref,
    pre_q_ref,
    pre_kv_ref,
    dec_q_ref,
    dec_kv_ref,
    cache_ref,
    pre_x_ref,
    dec_x_ref,
    ids_ref,
    logits_ref,
    out_ref,
    *rest,
    experts,
):
    pieces, x_ref = rest[:-1], rest[-1]
    attend(sinks_ref, len_ref, pre_q_ref, pre_kv_ref, dec_q_ref, dec_kv_ref, cache_ref, out_ref)
    line, core = line_ref[0], core_ref[0]
    half, width = x_ref.shape
    pre_rows = pre_x_ref.shape[0]
    second = jnp.concatenate(
        [pre_x_ref[half:pre_rows].astype(jnp.float32), dec_x_ref[...].astype(jnp.float32)], 0
    )
    x_ref[...] = jnp.where(core == 0, pre_x_ref[:half].astype(jnp.float32), second)
    topk, tokens = ids_ref.shape
    logits = [logits_ref[pl.ds(k, 1), :] for k in range(topk)]
    top = functools.reduce(jnp.maximum, logits)
    expo = [jnp.exp(value - top) for value in logits]
    total = functools.reduce(lambda a, b: a + b, expo)
    tail_width = pieces[0].shape[1] - width // len(pieces)
    place = lax.broadcasted_iota(jnp.int32, (tail_width, tokens), 0)
    factor = jnp.zeros((tail_width, tokens), jnp.float32)
    for k in range(topk):
        factor = factor + jnp.where(place % experts == ids_ref[pl.ds(k, 1), :], expo[k] / total, 0.0)
    high = factor.astype(jnp.bfloat16).astype(jnp.float32)
    factor = jnp.where(place < experts, high, jnp.where(place < 2 * experts, factor - high, 0.0))
    factor = factor.T
    tail = jnp.where(core == 0, factor[:half], factor[half:]).astype(jnp.bfloat16)
    share = width // len(pieces)
    for k, piece in enumerate(pieces):
        begin = pl.multiple_of(lax.rem(line + k, len(pieces)) * share, 128)
        piece[:, :share] = x_ref[:, pl.ds(begin, share)].astype(jnp.bfloat16)
        piece[:, share:] = tail


def attend(sinks_ref, len_ref, pre_q_ref, pre_kv_ref, dec_q_ref, dec_kv_ref, cache_ref, out_ref):
    pre_rows, q_width = pre_q_ref.shape
    dec_rows = dec_q_ref.shape[0]
    lanes = 2 * HEAD_SIZE
    group = (q_width // HEAD_SIZE) // (pre_kv_ref.shape[2] // HEAD_SIZE)
    scale = HEAD_SIZE ** (-0.5)
    padded = -(-pre_rows // 16) * 16
    positions = cache_ref.shape[2]

    def lane(rows):
        return lax.broadcasted_iota(jnp.int32, (rows, lanes), 1)

    def aligned(pair, side, head, rows):
        value = pair if side == head % 2 else pltpu.roll(pair, HEAD_SIZE, 1)
        return jnp.where((lane(rows) // HEAD_SIZE) == head % 2, value, 0.0)

    def joined(low, high, head, rows):
        low = low if head % 2 == 0 else pltpu.roll(low, HEAD_SIZE, 1)
        high = high if head % 2 == 1 else pltpu.roll(high, HEAD_SIZE, 1)
        return jnp.where(lane(rows) < HEAD_SIZE, low, high)

    def weights(scores, sink, more=None):
        top = jnp.maximum(jnp.max(scores, axis=-1, keepdims=True), sink)
        if more is not None:
            top = jnp.maximum(top, more)
        expo = jnp.exp(scores - top)
        total = jnp.sum(expo, axis=-1, keepdims=True) + jnp.exp(sink - top)
        if more is None:
            return (expo / total).astype(jnp.bfloat16), None
        extra = jnp.exp(more - top)
        total = total + extra
        return (expo / total).astype(jnp.bfloat16), (extra / total).astype(jnp.bfloat16)

    def filled(value):
        return jnp.concatenate(
            [value.astype(jnp.float32), jnp.zeros((padded - pre_rows, lanes), jnp.float32)], 0
        ).astype(jnp.bfloat16)

    contract = (((1,), (1,)), ((), ()))
    key_at = lax.broadcasted_iota(jnp.int32, (pre_rows, padded), 1)
    visible = key_at <= lax.broadcasted_iota(jnp.int32, (pre_rows, padded), 0)
    row_seq = lax.broadcasted_iota(jnp.int32, (dec_rows, positions), 0)
    length = jnp.zeros((dec_rows, positions), jnp.int32)
    for s in range(dec_rows):
        length = jnp.where(row_seq == s, len_ref[s], length)
    live = lax.broadcasted_iota(jnp.int32, (dec_rows, positions), 1) < length

    for head in range(pre_kv_ref.shape[2] // HEAD_SIZE):
        at_lanes = pl.ds((head // 2) * lanes, lanes)
        first_pair = head * group // 2
        here = range(first_pair, first_pair + group // 2)
        stacked = []
        for p in here:
            pair = pre_q_ref[:, pl.ds(p * lanes, lanes)].astype(jnp.float32)
            stacked += [aligned(pair, side, head, pre_rows) for side in (0, 1)]
        queries = jnp.concatenate(stacked, axis=0).astype(jnp.bfloat16)
        keys = filled(pre_kv_ref[0, :, at_lanes])
        scores = lax.dot_general(queries, keys, contract, preferred_element_type=jnp.float32)
        probs = []
        for i in range(group):
            block = scores[i * pre_rows : (i + 1) * pre_rows] * scale
            block = jnp.where(visible, block, -jnp.inf)
            probs.append(weights(block, sinks_ref[head * group + i])[0].astype(jnp.float32))
        pre_out = jnp.dot(
            jnp.concatenate(probs, axis=0).astype(jnp.bfloat16),
            filled(pre_kv_ref[1, :, at_lanes]),
            preferred_element_type=jnp.float32,
        )
        stacked = []
        for p in here:
            pair = dec_q_ref[:, pl.ds(p * lanes, lanes)].astype(jnp.float32)
            stacked += [aligned(pair, side, head, dec_rows) for side in (0, 1)]
        flat = jnp.concatenate(stacked, axis=0)
        queries = flat.astype(jnp.bfloat16)
        owner = lax.broadcasted_iota(jnp.int32, (group * dec_rows, positions), 0) % dec_rows
        past = jnp.zeros((group * dec_rows, positions), jnp.float32)
        for s in range(dec_rows):
            block = lax.dot_general(
                queries, cache_ref[0, s, :, at_lanes], contract, preferred_element_type=jnp.float32
            )
            past = jnp.where(owner == s, block, past)
        own_keys = dec_kv_ref[0, :, at_lanes].astype(jnp.float32)
        own_values = dec_kv_ref[1, :, at_lanes].astype(jnp.float32)
        probs, extras = [], []
        for i in range(group):
            rows = slice(i * dec_rows, (i + 1) * dec_rows)
            block = jnp.where(live, past[rows] * scale, -jnp.inf)
            own = jnp.sum(flat[rows] * own_keys, axis=1, keepdims=True) * scale
            prob, extra = weights(block, sinks_ref[head * group + i], own)
            probs.append(prob.astype(jnp.float32))
            extras.append(extra.astype(jnp.float32) * own_values)
        probs = jnp.concatenate(probs, axis=0)
        dec_out = jnp.concatenate(extras, axis=0)
        for s in range(dec_rows):
            dec_out = dec_out + jnp.dot(
                jnp.where(owner == s, probs, 0.0).astype(jnp.bfloat16),
                cache_ref[1, s, :, at_lanes],
                preferred_element_type=jnp.float32,
            )
        for n, p in enumerate(here):
            low, high = 2 * n, 2 * n + 1
            pre_pair = joined(
                pre_out[low * pre_rows : (low + 1) * pre_rows],
                pre_out[high * pre_rows : (high + 1) * pre_rows],
                head,
                pre_rows,
            )
            dec_pair = joined(
                dec_out[low * dec_rows : (low + 1) * dec_rows],
                dec_out[high * dec_rows : (high + 1) * dec_rows],
                head,
                dec_rows,
            )
            out_ref[:, pl.ds(p * lanes, lanes)] = jnp.concatenate([pre_pair, dec_pair], 0).astype(
                out_ref.dtype
            )


def attention(
    prefill_query_rows,
    prefill_key_values,
    decode_query_rows,
    decode_key_values,
    cache,
    cache_len,
    sinks,
):
    rows = prefill_query_rows.shape[0] + decode_query_rows.shape[0]
    width = prefill_query_rows.shape[1]
    scalars = pl.BlockSpec(memory_space=pltpu.SMEM)
    vectors = pl.BlockSpec(memory_space=pltpu.VMEM)
    return pl.pallas_call(
        attention_kernel,
        out_shape=jax.ShapeDtypeStruct((rows, width), jnp.bfloat16),
        in_specs=[scalars] * 2 + [vectors] * 5,
        out_specs=vectors,
        cost_estimate=pl.CostEstimate(
            flops=4_000_000_000, bytes_accessed=1_000_000, transcendentals=200_000
        ),
        compiler_params=pltpu.CompilerParams(vmem_limit_bytes=8 * 2**20),
        name="attention",
    )(
        sinks,
        cache_len,
        prefill_query_rows,
        prefill_key_values,
        decode_query_rows,
        decode_key_values,
        cache,
    )


def from_hbm(*values):
    return [pltpu.with_memory_space_constraint(v, pltpu.HBM) for v in values]


SCALARS = pl.BlockSpec(memory_space=pltpu.SMEM)
VECTORS = pl.BlockSpec(memory_space=pltpu.VMEM)


def start(where, inputs, x_pre, x_dec, expert_ids, route_logits, experts, deep):
    queries = inputs[0]
    rows = x_pre.shape[0] + x_dec.shape[0]
    half, width = rows // 2, x_pre.shape[1]
    piece = jax.ShapeDtypeStruct(
        (half, width // deep + -(-2 * experts // 128) * 128), jnp.bfloat16
    )
    pre_q, pre_kv, dec_q, dec_kv, cache, cache_len, sinks = inputs
    outs = pl.pallas_call(
        functools.partial(start_kernel, experts=experts),
        out_shape=[jax.ShapeDtypeStruct((rows, queries.shape[1]), jnp.bfloat16)] + [piece] * deep,
        in_specs=[SCALARS] * 6 + [VECTORS] * 9,
        out_specs=[VECTORS] * (deep + 1),
        scratch_shapes=[pltpu.VMEM((half, width), jnp.float32)],
        cost_estimate=pl.CostEstimate(
            flops=4_000_000_000, bytes_accessed=1_000_000, transcendentals=200_000
        ),
        compiler_params=pltpu.CompilerParams(vmem_limit_bytes=8 * 2**20),
        name="start",
    )(
        *where,
        *from_hbm(sinks, cache_len, pre_q, pre_kv, dec_q, dec_kv, cache, x_pre, x_dec),
        *from_hbm(expert_ids.T, route_logits.T),
    )
    return outs[0], outs[1:]


def project_kernel(core_ref, spot_ref, *refs, deep):
    attn = refs[:deep]
    columns, beside, across, kept_ref, given_ref, weight_ref = refs[deep:]
    core, spot = core_ref[0], spot_ref[0]
    count = columns.shape[0]
    for near in range(PLANE):
        other = (near >> 1) | ((near & 1) << 1)
        chip = jnp.bitwise_xor(spot, jnp.where(core == 0, near, other))
        block = (columns, beside, across.at[0], across.at[1])[near]
        weight_ref[pl.ds(pl.multiple_of(chip * count, 16), count), :] = block[...]
    half = kept_ref.shape[1]
    parts = lax.dot_general(
        jnp.concatenate([block[...] for block in attn], axis=0),
        weight_ref[...],
        (((1,), (1,)), ((), ())),
        preferred_element_type=jnp.float32,
    )
    for k in range(deep):
        part = parts[2 * half * k : 2 * half * (k + 1)]
        kept_ref[k] = jnp.where(core == 0, part[:half], part[half:])
        given_ref[k] = jnp.where(core == 0, part[half:], part[:half])


def project(core_at, spot_at, attn, columns, beside, across):
    deep, half = len(attn), attn[0].shape[0] // 2
    share = PLANE * columns.shape[0]
    blocks = pltpu.VMEM((deep, half, share), jnp.float32)
    return pl.pallas_call(
        functools.partial(project_kernel, deep=deep),
        out_shape=[blocks, blocks],
        in_specs=[SCALARS] * 2 + [VECTORS] * (deep + 3),
        out_specs=[VECTORS] * 2,
        scratch_shapes=[pltpu.VMEM((share, columns.shape[1]), jnp.bfloat16)],
        cost_estimate=pl.CostEstimate(
            flops=4 * deep * half * share * columns.shape[1],
            bytes_accessed=2_000_000,
            transcendentals=0,
        ),
        compiler_params=pltpu.CompilerParams(vmem_limit_bytes=8 * 2**20),
        name="project",
    )(core_at, spot_at, *attn, columns, beside, across)


def slot_count(tokens_here, topk, experts):
    return min(
        tokens_here, 2 * ((3 * max(1, (tokens_here * topk + experts - 1) // experts) + 3) // 4)
    )


def slot_plan(
    attn_rows, resid, o_weight, norm_gain, expert_ids, route_logits, w_gate_up, w_down
):
    width = resid.shape[1]
    half = attn_rows.shape[0] // 2
    mine = lax.axis_index("hp") * half
    head_part = jnp.dot(
        attn_rows,
        lax.all_gather(o_weight, "ep", axis=1, tiled=True),
        preferred_element_type=jnp.float32,
    )
    summed = lax.psum_scatter(head_part, "hp", scatter_dimension=0, tiled=True)
    stream = lax.dynamic_slice_in_dim(resid, mine, half, 0).astype(jnp.float32) + summed
    normed = lax.all_gather(rms_norm(stream, norm_gain), "hp", axis=0, tiled=True)
    tokens_here, topk = expert_ids.shape
    holders = lax.axis_size("ep")
    experts = holders // 2
    slot = slot_count(tokens_here, topk, experts)
    plane = slot // 2
    flat_ids = expert_ids.reshape(-1)
    onehot = (flat_ids[:, None] == jnp.arange(experts, dtype=jnp.int32)[None, :]).astype(jnp.int32)
    rank = jnp.sum(jnp.cumsum(onehot, axis=0) * onehot, axis=1) - 1
    position = (flat_ids * slot + rank).reshape(tokens_here, topk)
    columns = jnp.arange(experts * slot, dtype=jnp.int32)[None, None, :] == position[:, :, None]
    picked_rows = jnp.any(columns, axis=1).T.astype(jnp.bfloat16)
    per_expert = (
        jnp.dot(picked_rows, normed, preferred_element_type=jnp.float32)
        .astype(jnp.bfloat16)
        .reshape(experts, slot, width)
    )
    send = jnp.repeat(per_expert, 2, axis=0)
    own_plane = lax.dynamic_slice_in_dim(send, lax.axis_index("hp") * plane, plane, 1)
    arrived_plane = lax.all_to_all(own_plane, "ep", split_axis=0, concat_axis=0, tiled=True)
    arrived = lax.all_gather(arrived_plane, "hp", axis=1, tiled=True)
    rows = arrived.reshape(-1, width)
    gate = jnp.dot(rows, w_gate_up[0, 0], preferred_element_type=jnp.float32)
    upper = jnp.dot(rows, w_gate_up[0, 1], preferred_element_type=jnp.float32)
    hidden = ((upper + 1.0) * gate * jax.nn.sigmoid(1.702 * gate)).astype(jnp.bfloat16)
    partial_out = jnp.dot(hidden, w_down[0], preferred_element_type=jnp.float32).reshape(
        -1, slot, width
    )
    share = lax.psum_scatter(
        partial_out.astype(jnp.bfloat16), "hp", scatter_dimension=1, tiled=True
    )
    returned = lax.all_to_all(share, "ep", split_axis=0, concat_axis=0, tiled=True)
    mix = jax.nn.softmax(route_logits, axis=-1)
    blend = jnp.sum(jnp.where(columns, mix[:, :, None], 0.0), axis=1).reshape(
        tokens_here, experts, slot
    )
    blend = jnp.repeat(blend, 2, axis=1)
    blend_plane = lax.dynamic_slice_in_dim(blend, lax.axis_index("hp") * plane, plane, 2).reshape(
        tokens_here, holders * plane
    )
    terms = jnp.dot(
        blend_plane,
        returned.reshape(-1, width).astype(jnp.float32),
        precision=lax.Precision.HIGHEST,
    )
    moe = lax.psum_scatter(
        terms.astype(jnp.bfloat16), "hp", scatter_dimension=0, tiled=True
    ).astype(jnp.float32)
    return (stream + moe).astype(jnp.bfloat16)


def pack_kernel(gate_up_a, gate_up_b, down_a, down_b, gate_up_ref, down_ref, sems):
    units = down_a.shape[0]
    copies = [
        pltpu.make_async_copy(gate_up_a, gate_up_ref.at[:, :, :units], sems.at[0]),
        pltpu.make_async_copy(gate_up_b, gate_up_ref.at[:, :, units:], sems.at[1]),
        pltpu.make_async_copy(down_a, down_ref.at[:units], sems.at[2]),
        pltpu.make_async_copy(down_b, down_ref.at[units:], sems.at[3]),
    ]
    for copy in copies:
        copy.start()
    for copy in copies:
        copy.wait()


def pack(gate_up_a, gate_up_b, down_a, down_b):
    units, width = down_a.shape
    kinds = gate_up_a.dtype
    return pl.pallas_call(
        pack_kernel,
        out_shape=[pltpu.VMEM((2, width, 2 * units), kinds), pltpu.VMEM((2 * units, width), kinds)],
        in_specs=[pl.BlockSpec(memory_space=pltpu.HBM)] * 4,
        out_specs=[VECTORS] * 2,
        scratch_shapes=[pltpu.SemaphoreType.DMA((4,))],
        cost_estimate=pl.CostEstimate(
            flops=2_000_000_000, bytes_accessed=12 * width * units, transcendentals=0
        ),
        compiler_params=pltpu.CompilerParams(vmem_limit_bytes=10 * 2**20),
        name="pack",
    )(gate_up_a, gate_up_b, down_a, down_b)


def held_kernel(value_ref, out_ref):
    out_ref[...] = value_ref[...]


def held(value):
    return pl.pallas_call(
        held_kernel,
        out_shape=pltpu.VMEM(value.shape, value.dtype),
        in_specs=[VECTORS],
        out_specs=VECTORS,
        cost_estimate=pl.CostEstimate(flops=1_000_000, bytes_accessed=10_000, transcendentals=0),
        compiler_params=pltpu.CompilerParams(vmem_limit_bytes=2**20),
        name="held",
    )(value)


def expert_kernel(
    mine_ref, line_ref, gain_ref, first, second, others, gate_up, down, out_ref, inputs_ref, *, experts
):
    width, share = gate_up.shape[1], second.shape[1]
    deep, line = width // share, line_ref[0]
    blocks = [first[:, :share], second[...]] + [others[i] for i in range(deep - 2)]
    blocks = [block.astype(jnp.float32) for block in blocks]
    square = functools.reduce(lambda x, y: x + y, [block * block for block in blocks])
    root = lax.rsqrt(jnp.sum(square, axis=-1, keepdims=True) * (1.0 / width) + EPS)
    for b, block in enumerate(blocks):
        columns = pl.ds(pl.multiple_of(lax.rem(line + deep - b, deep) * share, 128), share)
        inputs_ref[:, columns] = (block * root * gain_ref[:, columns]).astype(jnp.bfloat16)
    inputs = inputs_ref[...]
    tail = first[:, share:].astype(jnp.float32)
    lanes = lax.broadcasted_iota(jnp.int32, tail.shape, 1)
    mine = mine_ref[0]
    scale = jnp.sum(
        jnp.where((lanes == mine) | (lanes == mine + experts), tail, 0.0), 1, keepdims=True
    )
    gate = jnp.dot(inputs, gate_up[0], preferred_element_type=jnp.float32)
    upper = jnp.dot(inputs, gate_up[1], preferred_element_type=jnp.float32)
    hidden = ((upper + 1.0) * gate * jax.nn.sigmoid(1.702 * gate)).astype(jnp.bfloat16)
    total = jnp.dot(hidden, down[...], preferred_element_type=jnp.float32)
    out_ref[...] = (total * scale).astype(out_ref.dtype)


def expert_rows(mine_at, line_at, gain, groups, weights, experts, out_type):
    count, (units, width) = groups[0].shape[0], weights[1].shape
    return pl.pallas_call(
        functools.partial(expert_kernel, experts=experts),
        out_shape=pltpu.VMEM((count, width), out_type),
        in_specs=[SCALARS] * 2 + [VECTORS] * 6,
        out_specs=VECTORS,
        scratch_shapes=[pltpu.VMEM((count, width), jnp.bfloat16)],
        cost_estimate=pl.CostEstimate(
            flops=6 * count * width * units,
            bytes_accessed=6 * width * units,
            transcendentals=count * units,
        ),
        compiler_params=pltpu.CompilerParams(vmem_limit_bytes=12 * 2**20),
        name="expert",
    )(mine_at, line_at, gain, *groups, *weights)


def finish_kernel(line_ref, own_ref, near_ref, over_ref, *refs, deep):
    blocks, rest_ref, sent = refs[:deep], refs[deep], refs[deep + 1 :]
    half, share, line = rest_ref.shape[0], blocks[0].shape[2], line_ref[0]
    for c in range(deep):
        rows = pl.ds(c * half, half)
        total = own_ref[rows, :] + near_ref[rows, :].astype(jnp.float32)
        total = total + over_ref[rows, :].astype(jnp.float32)
        if c == 0:
            rest_ref[...] = total
        else:
            sent[deep - c - 1][...] = total.astype(jnp.bfloat16)
    for b, block in enumerate(blocks):
        columns = pl.ds(pl.multiple_of(lax.rem(line + deep - b, deep) * share, 128), share)
        rest_ref[:, columns] += block[(deep - b) % deep].astype(jnp.float32)


def finish(line_at, own, near_back, over, blocks):
    deep, half, share = blocks[0].shape
    width = deep * share
    return pl.pallas_call(
        functools.partial(finish_kernel, deep=deep),
        out_shape=[pltpu.VMEM((half, width), jnp.float32)]
        + [pltpu.VMEM((half, width), jnp.bfloat16)] * (deep - 1),
        in_specs=[SCALARS] + [VECTORS] * (3 + deep),
        out_specs=[VECTORS] * deep,
        cost_estimate=pl.CostEstimate(
            flops=500_000_000, bytes_accessed=1_000_000, transcendentals=0
        ),
        compiler_params=pltpu.CompilerParams(vmem_limit_bytes=8 * 2**20),
        name="finish",
    )(line_at, own, near_back, over, *blocks)


PLANE = 4


def plane_perm(holders, stage):
    return [
        (2 * e + h, 2 * (e ^ (1 if h == stage else 2)) + h) for e in range(holders) for h in (0, 1)
    ]


def line_perm(holders, step):
    return [(e, (e + PLANE * step) % holders) for e in range(holders)]


def dense_plan(
    inputs, x_pre, x_dec, o_weight, norm_gain, expert_ids, route_logits, w_gate_up, w_down
):
    width = x_pre.shape[1]
    holders = lax.axis_size("ep")
    experts = holders // 2
    deep = holders // PLANE
    place, core = lax.axis_index("ep"), lax.axis_index("hp")
    line, spot = place // PLANE, place % PLANE
    swap = [(0, 1), (1, 0)]
    far_first = range(deep - 1, 0, -1)
    where = [jnp.reshape(v, (1,)).astype(jnp.int32) for v in (line, core, spot, place // 2)]
    line_at, core_at, spot_at, mine_at = where

    def plane(value, stage):
        return lax.ppermute(value, ("ep", "hp"), plane_perm(holders, stage))

    def along(value, step):
        return lax.ppermute(value, "ep", line_perm(holders, step))

    def gather_line(value):
        got = {k: along(value, k) for k in far_first}
        return [value] + [got[k] for k in range(1, deep)]

    gate_up_here, down_here = w_gate_up[0], w_down[0]
    gate_up_there = lax.ppermute(gate_up_here, "hp", swap)
    down_there = lax.ppermute(down_here, "hp", swap)

    weights = pack(gate_up_here, gate_up_there, down_here, down_there)

    columns = o_weight.T
    beside = plane(columns, 0)
    across = plane(jnp.stack([columns, beside]), 1)

    attn_rows, pieces = start(where, inputs, x_pre, x_dec, expert_ids, route_logits, experts, deep)
    attn = gather_line(attn_rows)
    arrived = {k: along(pieces[k], k) for k in far_first}
    arrived[0] = pieces[0]
    pieces = [arrived[k] for k in range(deep)]
    kept, given = project(core_at, spot_at, attn, columns, beside, across)
    added = jnp.stack([piece[:, : kept.shape[2]] for piece in pieces]).astype(jnp.float32)
    summed = (kept + lax.ppermute(given, "hp", swap) + added).astype(jnp.bfloat16)
    blocks = gather_line(summed)

    def back_from_here(block, back):
        turned = [block[(c - back) % deep] for c in range(deep)]
        return jnp.concatenate(turned, axis=0)

    columns_of = [back_from_here(block, b) for b, block in enumerate(blocks)]
    tails = jnp.concatenate([piece[:, kept.shape[2] :] for piece in pieces], axis=0)
    groups = [
        jnp.concatenate([columns_of[0], tails], axis=1),
        columns_of[1],
        jnp.stack(columns_of[2:]),
    ]
    parts = range(len(groups))
    gain = held(norm_gain.reshape(1, width))

    def expert(groups, out_type):
        return expert_rows(mine_at, line_at, gain, groups, weights, experts, out_type)

    near_groups = [plane(groups[i], 0) for i in parts]
    both_groups = [plane(near_groups[i], 1) for i in parts]
    far_groups = [plane(groups[i], 1) for i in parts]
    own = expert(groups, jnp.float32)
    near_out = expert(near_groups, jnp.bfloat16)
    both_out = expert(both_groups, jnp.bfloat16)
    far_out = expert(far_groups, jnp.float32)
    far_back = plane(both_out, 0)
    near_back = plane(near_out, 0)
    over = plane((far_out + far_back.astype(jnp.float32)).astype(jnp.bfloat16), 1)
    rest, *sent = finish(line_at, own, near_back, over, blocks)
    got = [along(sent[k - 1], k) for k in far_first]
    for block in got:
        rest = rest + block.astype(jnp.float32)
    return rest.astype(jnp.bfloat16)


def on_device(
    x_pre,
    x_dec,
    prefill_query_rows,
    prefill_key_values,
    decode_query_rows,
    decode_key_values,
    cache,
    cache_len,
    sinks,
    o_weight,
    norm_gain,
    expert_ids,
    route_logits,
    w_gate_up,
    w_down,
):
    inputs = (
        prefill_query_rows,
        prefill_key_values,
        decode_query_rows,
        decode_key_values,
        cache,
        cache_len,
        sinks,
    )
    rest = (o_weight, norm_gain, expert_ids, route_logits, w_gate_up, w_down)
    tokens_here, topk = expert_ids.shape
    holders = lax.axis_size("ep")
    dense = tokens_here <= 2 * slot_count(tokens_here, topk, holders // 2)
    even = holders % PLANE == 0 and holders >= 3 * PLANE and x_pre.shape[1] % (holders // PLANE * 128) == 0
    if dense and even and lax.axis_size("hp") == 2:
        return dense_plan(inputs, x_pre, x_dec, *rest)
    return slot_plan(attention(*inputs), jnp.concatenate([x_pre, x_dec], axis=0), *rest)


def solution(mesh):
    placed = (
        P(("groups", "ep"), None),
        P(("groups", "ep"), None),
        P(("groups", "ep"), "hp"),
        P(None, ("groups", "ep"), "hp"),
        P(("groups", "ep"), "hp"),
        P(None, ("groups", "ep"), "hp"),
        P(None, ("groups", "ep"), None, "hp"),
        P(("groups", "ep")),
        P("hp"),
        P("hp", "ep"),
        P(),
        P(("groups", "ep"), None),
        P(("groups", "ep"), None),
        P("ep", None, None, "hp"),
        P("ep", "hp", None),
    )
    return jax.shard_map(
        on_device,
        mesh=mesh,
        in_specs=placed,
        out_specs=P(("groups", "ep", "hp"), None),
        check_vma=False,
    )
```

```python
import functools
import jax
import jax.numpy as jnp
from jax import lax
from jax.experimental import pallas as pl
from jax.experimental.pallas import tpu as pltpu
from jax.sharding import PartitionSpec as P


HEAD_SIZE = 64


EPS = 1e-05


def rms_norm(stream, gain):
    mean_sq = jnp.mean(stream * stream, axis=-1, keepdims=True)
    return (stream * lax.rsqrt(mean_sq + EPS) * gain).astype(jnp.bfloat16)


def attention_kernel(
    sinks_ref, len_ref, pre_q_ref, pre_kv_ref, dec_q_ref, dec_kv_ref, cache_ref, out_ref
):
    attend(sinks_ref, len_ref, pre_q_ref, pre_kv_ref, dec_q_ref, dec_kv_ref, cache_ref, out_ref)


def start_kernel(
    line_ref,
    core_ref,
    spot_ref,
    mine_ref,
    sinks_ref,
    len_ref,
    pre_q_ref,
    pre_kv_ref,
    dec_q_ref,
    dec_kv_ref,
    cache_ref,
    pre_x_ref,
    dec_x_ref,
    ids_ref,
    logits_ref,
    out_ref,
    *rest,
    experts,
):
    pieces, x_ref = rest[:-1], rest[-1]
    attend(sinks_ref, len_ref, pre_q_ref, pre_kv_ref, dec_q_ref, dec_kv_ref, cache_ref, out_ref)
    line, core = line_ref[0], core_ref[0]
    half, width = x_ref.shape
    pre_rows = pre_x_ref.shape[0]
    second = jnp.concatenate(
        [pre_x_ref[half:pre_rows].astype(jnp.float32), dec_x_ref[...].astype(jnp.float32)], 0
    )
    x_ref[...] = jnp.where(core == 0, pre_x_ref[:half].astype(jnp.float32), second)
    topk, tokens = ids_ref.shape
    logits = [logits_ref[pl.ds(k, 1), :] for k in range(topk)]
    top = functools.reduce(jnp.maximum, logits)
    expo = [jnp.exp(value - top) for value in logits]
    total = functools.reduce(lambda a, b: a + b, expo)
    tail_width = pieces[0].shape[1] - width // len(pieces)
    place = lax.broadcasted_iota(jnp.int32, (tail_width, tokens), 0)
    factor = jnp.zeros((tail_width, tokens), jnp.float32)
    for k in range(topk):
        factor = factor + jnp.where(place % experts == ids_ref[pl.ds(k, 1), :], expo[k] / total, 0.0)
    high = factor.astype(jnp.bfloat16).astype(jnp.float32)
    factor = jnp.where(place < experts, high, jnp.where(place < 2 * experts, factor - high, 0.0))
    factor = factor.T
    tail = jnp.where(core == 0, factor[:half], factor[half:]).astype(jnp.bfloat16)
    share = width // len(pieces)
    for k, piece in enumerate(pieces):
        begin = pl.multiple_of(lax.rem(line + k, len(pieces)) * share, 128)
        piece[:, :share] = x_ref[:, pl.ds(begin, share)].astype(jnp.bfloat16)
        piece[:, share:] = tail


def attend(sinks_ref, len_ref, pre_q_ref, pre_kv_ref, dec_q_ref, dec_kv_ref, cache_ref, out_ref):
    pre_rows, q_width = pre_q_ref.shape
    dec_rows = dec_q_ref.shape[0]
    lanes = 2 * HEAD_SIZE
    group = (q_width // HEAD_SIZE) // (pre_kv_ref.shape[2] // HEAD_SIZE)
    scale = HEAD_SIZE ** (-0.5)
    padded = -(-pre_rows // 16) * 16
    positions = cache_ref.shape[2]

    def lane(rows):
        return lax.broadcasted_iota(jnp.int32, (rows, lanes), 1)

    def aligned(pair, side, head, rows):
        value = pair if side == head % 2 else pltpu.roll(pair, HEAD_SIZE, 1)
        return jnp.where((lane(rows) // HEAD_SIZE) == head % 2, value, 0.0)

    def joined(low, high, head, rows):
        low = low if head % 2 == 0 else pltpu.roll(low, HEAD_SIZE, 1)
        high = high if head % 2 == 1 else pltpu.roll(high, HEAD_SIZE, 1)
        return jnp.where(lane(rows) < HEAD_SIZE, low, high)

    def weights(scores, sink, more=None):
        top = jnp.maximum(jnp.max(scores, axis=-1, keepdims=True), sink)
        if more is not None:
            top = jnp.maximum(top, more)
        expo = jnp.exp(scores - top)
        total = jnp.sum(expo, axis=-1, keepdims=True) + jnp.exp(sink - top)
        if more is None:
            return (expo / total).astype(jnp.bfloat16), None
        extra = jnp.exp(more - top)
        total = total + extra
        return (expo / total).astype(jnp.bfloat16), (extra / total).astype(jnp.bfloat16)

    def filled(value):
        return jnp.concatenate(
            [value.astype(jnp.float32), jnp.zeros((padded - pre_rows, lanes), jnp.float32)], 0
        ).astype(jnp.bfloat16)

    contract = (((1,), (1,)), ((), ()))
    key_at = lax.broadcasted_iota(jnp.int32, (pre_rows, padded), 1)
    visible = key_at <= lax.broadcasted_iota(jnp.int32, (pre_rows, padded), 0)
    row_seq = lax.broadcasted_iota(jnp.int32, (dec_rows, positions), 0)
    length = jnp.zeros((dec_rows, positions), jnp.int32)
    for s in range(dec_rows):
        length = jnp.where(row_seq == s, len_ref[s], length)
    live = lax.broadcasted_iota(jnp.int32, (dec_rows, positions), 1) < length

    for head in range(pre_kv_ref.shape[2] // HEAD_SIZE):
        at_lanes = pl.ds((head // 2) * lanes, lanes)
        first_pair = head * group // 2
        here = range(first_pair, first_pair + group // 2)
        stacked = []
        for p in here:
            pair = pre_q_ref[:, pl.ds(p * lanes, lanes)].astype(jnp.float32)
            stacked += [aligned(pair, side, head, pre_rows) for side in (0, 1)]
        queries = jnp.concatenate(stacked, axis=0).astype(jnp.bfloat16)
        keys = filled(pre_kv_ref[0, :, at_lanes])
        scores = lax.dot_general(queries, keys, contract, preferred_element_type=jnp.float32)
        probs = []
        for i in range(group):
            block = scores[i * pre_rows : (i + 1) * pre_rows] * scale
            block = jnp.where(visible, block, -jnp.inf)
            probs.append(weights(block, sinks_ref[head * group + i])[0].astype(jnp.float32))
        pre_out = jnp.dot(
            jnp.concatenate(probs, axis=0).astype(jnp.bfloat16),
            filled(pre_kv_ref[1, :, at_lanes]),
            preferred_element_type=jnp.float32,
        )
        stacked = []
        for p in here:
            pair = dec_q_ref[:, pl.ds(p * lanes, lanes)].astype(jnp.float32)
            stacked += [aligned(pair, side, head, dec_rows) for side in (0, 1)]
        flat = jnp.concatenate(stacked, axis=0)
        queries = flat.astype(jnp.bfloat16)
        owner = lax.broadcasted_iota(jnp.int32, (group * dec_rows, positions), 0) % dec_rows
        past = jnp.zeros((group * dec_rows, positions), jnp.float32)
        for s in range(dec_rows):
            block = lax.dot_general(
                queries, cache_ref[0, s, :, at_lanes], contract, preferred_element_type=jnp.float32
            )
            past = jnp.where(owner == s, block, past)
        own_keys = dec_kv_ref[0, :, at_lanes].astype(jnp.float32)
        own_values = dec_kv_ref[1, :, at_lanes].astype(jnp.float32)
        probs, extras = [], []
        for i in range(group):
            rows = slice(i * dec_rows, (i + 1) * dec_rows)
            block = jnp.where(live, past[rows] * scale, -jnp.inf)
            own = jnp.sum(flat[rows] * own_keys, axis=1, keepdims=True) * scale
            prob, extra = weights(block, sinks_ref[head * group + i], own)
            probs.append(prob.astype(jnp.float32))
            extras.append(extra.astype(jnp.float32) * own_values)
        probs = jnp.concatenate(probs, axis=0)
        dec_out = jnp.concatenate(extras, axis=0)
        for s in range(dec_rows):
            dec_out = dec_out + jnp.dot(
                jnp.where(owner == s, probs, 0.0).astype(jnp.bfloat16),
                cache_ref[1, s, :, at_lanes],
                preferred_element_type=jnp.float32,
            )
        for n, p in enumerate(here):
            low, high = 2 * n, 2 * n + 1
            pre_pair = joined(
                pre_out[low * pre_rows : (low + 1) * pre_rows],
                pre_out[high * pre_rows : (high + 1) * pre_rows],
                head,
                pre_rows,
            )
            dec_pair = joined(
                dec_out[low * dec_rows : (low + 1) * dec_rows],
                dec_out[high * dec_rows : (high + 1) * dec_rows],
                head,
                dec_rows,
            )
            out_ref[:, pl.ds(p * lanes, lanes)] = jnp.concatenate([pre_pair, dec_pair], 0).astype(
                out_ref.dtype
            )


def attention(
    prefill_query_rows,
    prefill_key_values,
    decode_query_rows,
    decode_key_values,
    cache,
    cache_len,
    sinks,
):
    rows = prefill_query_rows.shape[0] + decode_query_rows.shape[0]
    width = prefill_query_rows.shape[1]
    scalars = pl.BlockSpec(memory_space=pltpu.SMEM)
    vectors = pl.BlockSpec(memory_space=pltpu.VMEM)
    return pl.pallas_call(
        attention_kernel,
        out_shape=jax.ShapeDtypeStruct((rows, width), jnp.bfloat16),
        in_specs=[scalars] * 2 + [vectors] * 5,
        out_specs=vectors,
        cost_estimate=pl.CostEstimate(
            flops=4_000_000_000, bytes_accessed=1_000_000, transcendentals=200_000
        ),
        compiler_params=pltpu.CompilerParams(vmem_limit_bytes=8 * 2**20),
        name="attention",
    )(
        sinks,
        cache_len,
        prefill_query_rows,
        prefill_key_values,
        decode_query_rows,
        decode_key_values,
        cache,
    )


def from_hbm(*values):
    return [pltpu.with_memory_space_constraint(v, pltpu.HBM) for v in values]


SCALARS = pl.BlockSpec(memory_space=pltpu.SMEM)
VECTORS = pl.BlockSpec(memory_space=pltpu.VMEM)


def start(where, inputs, x_pre, x_dec, expert_ids, route_logits, experts, deep):
    queries = inputs[0]
    rows = x_pre.shape[0] + x_dec.shape[0]
    half, width = rows // 2, x_pre.shape[1]
    piece = jax.ShapeDtypeStruct(
        (half, width // deep + -(-2 * experts // 128) * 128), jnp.bfloat16
    )
    pre_q, pre_kv, dec_q, dec_kv, cache, cache_len, sinks = inputs
    outs = pl.pallas_call(
        functools.partial(start_kernel, experts=experts),
        out_shape=[jax.ShapeDtypeStruct((rows, queries.shape[1]), jnp.bfloat16)] + [piece] * deep,
        in_specs=[SCALARS] * 6 + [VECTORS] * 9,
        out_specs=[VECTORS] * (deep + 1),
        scratch_shapes=[pltpu.VMEM((half, width), jnp.float32)],
        cost_estimate=pl.CostEstimate(
            flops=4_000_000_000, bytes_accessed=1_000_000, transcendentals=200_000
        ),
        compiler_params=pltpu.CompilerParams(vmem_limit_bytes=8 * 2**20),
        name="start",
    )(
        *where,
        *from_hbm(sinks, cache_len, pre_q, pre_kv, dec_q, dec_kv, cache, x_pre, x_dec),
        *from_hbm(expert_ids.T, route_logits.T),
    )
    return outs[0], outs[1:]


def project_kernel(core_ref, spot_ref, *refs, deep):
    attn = refs[:deep]
    columns, beside, across, kept_ref, given_ref, weight_ref = refs[deep:]
    core, spot = core_ref[0], spot_ref[0]
    count = columns.shape[0]
    for near in range(PLANE):
        other = (near >> 1) | ((near & 1) << 1)
        chip = jnp.bitwise_xor(spot, jnp.where(core == 0, near, other))
        block = (columns, beside, across.at[0], across.at[1])[near]
        weight_ref[pl.ds(pl.multiple_of(chip * count, 16), count), :] = block[...]
    half = kept_ref.shape[1]
    parts = lax.dot_general(
        jnp.concatenate([block[...] for block in attn], axis=0),
        weight_ref[...],
        (((1,), (1,)), ((), ())),
        preferred_element_type=jnp.float32,
    )
    for k in range(deep):
        part = parts[2 * half * k : 2 * half * (k + 1)]
        kept_ref[k] = jnp.where(core == 0, part[:half], part[half:])
        given_ref[k] = jnp.where(core == 0, part[half:], part[:half])


def project(core_at, spot_at, attn, columns, beside, across):
    deep, half = len(attn), attn[0].shape[0] // 2
    share = PLANE * columns.shape[0]
    blocks = pltpu.VMEM((deep, half, share), jnp.float32)
    return pl.pallas_call(
        functools.partial(project_kernel, deep=deep),
        out_shape=[blocks, blocks],
        in_specs=[SCALARS] * 2 + [VECTORS] * (deep + 3),
        out_specs=[VECTORS] * 2,
        scratch_shapes=[pltpu.VMEM((share, columns.shape[1]), jnp.bfloat16)],
        cost_estimate=pl.CostEstimate(
            flops=4 * deep * half * share * columns.shape[1],
            bytes_accessed=2_000_000,
            transcendentals=0,
        ),
        compiler_params=pltpu.CompilerParams(vmem_limit_bytes=8 * 2**20),
        name="project",
    )(core_at, spot_at, *attn, columns, beside, across)


def slot_count(tokens_here, topk, experts):
    return min(
        tokens_here, 2 * ((3 * max(1, (tokens_here * topk + experts - 1) // experts) + 3) // 4)
    )


def slot_plan(
    attn_rows, resid, o_weight, norm_gain, expert_ids, route_logits, w_gate_up, w_down
):
    width = resid.shape[1]
    half = attn_rows.shape[0] // 2
    mine = lax.axis_index("hp") * half
    head_part = jnp.dot(
        attn_rows,
        lax.all_gather(o_weight, "ep", axis=1, tiled=True),
        preferred_element_type=jnp.float32,
    )
    summed = lax.psum_scatter(head_part, "hp", scatter_dimension=0, tiled=True)
    stream = lax.dynamic_slice_in_dim(resid, mine, half, 0).astype(jnp.float32) + summed
    normed = lax.all_gather(rms_norm(stream, norm_gain), "hp", axis=0, tiled=True)
    tokens_here, topk = expert_ids.shape
    holders = lax.axis_size("ep")
    experts = holders // 2
    slot = slot_count(tokens_here, topk, experts)
    plane = slot // 2
    flat_ids = expert_ids.reshape(-1)
    onehot = (flat_ids[:, None] == jnp.arange(experts, dtype=jnp.int32)[None, :]).astype(jnp.int32)
    rank = jnp.sum(jnp.cumsum(onehot, axis=0) * onehot, axis=1) - 1
    position = (flat_ids * slot + rank).reshape(tokens_here, topk)
    columns = jnp.arange(experts * slot, dtype=jnp.int32)[None, None, :] == position[:, :, None]
    picked_rows = jnp.any(columns, axis=1).T.astype(jnp.bfloat16)
    per_expert = (
        jnp.dot(picked_rows, normed, preferred_element_type=jnp.float32)
        .astype(jnp.bfloat16)
        .reshape(experts, slot, width)
    )
    send = jnp.repeat(per_expert, 2, axis=0)
    own_plane = lax.dynamic_slice_in_dim(send, lax.axis_index("hp") * plane, plane, 1)
    arrived_plane = lax.all_to_all(own_plane, "ep", split_axis=0, concat_axis=0, tiled=True)
    arrived = lax.all_gather(arrived_plane, "hp", axis=1, tiled=True)
    rows = arrived.reshape(-1, width)
    gate = jnp.dot(rows, w_gate_up[0, 0], preferred_element_type=jnp.float32)
    upper = jnp.dot(rows, w_gate_up[0, 1], preferred_element_type=jnp.float32)
    hidden = ((upper + 1.0) * gate * jax.nn.sigmoid(1.702 * gate)).astype(jnp.bfloat16)
    partial_out = jnp.dot(hidden, w_down[0], preferred_element_type=jnp.float32).reshape(
        -1, slot, width
    )
    share = lax.psum_scatter(
        partial_out.astype(jnp.bfloat16), "hp", scatter_dimension=1, tiled=True
    )
    returned = lax.all_to_all(share, "ep", split_axis=0, concat_axis=0, tiled=True)
    mix = jax.nn.softmax(route_logits, axis=-1)
    blend = jnp.sum(jnp.where(columns, mix[:, :, None], 0.0), axis=1).reshape(
        tokens_here, experts, slot
    )
    blend = jnp.repeat(blend, 2, axis=1)
    blend_plane = lax.dynamic_slice_in_dim(blend, lax.axis_index("hp") * plane, plane, 2).reshape(
        tokens_here, holders * plane
    )
    terms = jnp.dot(
        blend_plane,
        returned.reshape(-1, width).astype(jnp.float32),
        precision=lax.Precision.HIGHEST,
    )
    moe = lax.psum_scatter(
        terms.astype(jnp.bfloat16), "hp", scatter_dimension=0, tiled=True
    ).astype(jnp.float32)
    return (stream + moe).astype(jnp.bfloat16)


def pack_kernel(gate_up_a, gate_up_b, down_a, down_b, gate_up_ref, down_ref, sems):
    units = down_a.shape[0]
    copies = [
        pltpu.make_async_copy(gate_up_a, gate_up_ref.at[:, :, :units], sems.at[0]),
        pltpu.make_async_copy(gate_up_b, gate_up_ref.at[:, :, units:], sems.at[1]),
        pltpu.make_async_copy(down_a, down_ref.at[:units], sems.at[2]),
        pltpu.make_async_copy(down_b, down_ref.at[units:], sems.at[3]),
    ]
    for copy in copies:
        copy.start()
    for copy in copies:
        copy.wait()


def pack(gate_up_a, gate_up_b, down_a, down_b):
    units, width = down_a.shape
    kinds = gate_up_a.dtype
    return pl.pallas_call(
        pack_kernel,
        out_shape=[pltpu.VMEM((2, width, 2 * units), kinds), pltpu.VMEM((2 * units, width), kinds)],
        in_specs=[pl.BlockSpec(memory_space=pltpu.HBM)] * 4,
        out_specs=[VECTORS] * 2,
        scratch_shapes=[pltpu.SemaphoreType.DMA((4,))],
        cost_estimate=pl.CostEstimate(
            flops=2_000_000_000, bytes_accessed=12 * width * units, transcendentals=0
        ),
        compiler_params=pltpu.CompilerParams(vmem_limit_bytes=10 * 2**20),
        name="pack",
    )(gate_up_a, gate_up_b, down_a, down_b)


def held_kernel(value_ref, out_ref):
    out_ref[...] = value_ref[...]


def held(value):
    return pl.pallas_call(
        held_kernel,
        out_shape=pltpu.VMEM(value.shape, value.dtype),
        in_specs=[VECTORS],
        out_specs=VECTORS,
        cost_estimate=pl.CostEstimate(flops=1_000_000, bytes_accessed=10_000, transcendentals=0),
        compiler_params=pltpu.CompilerParams(vmem_limit_bytes=2**20),
        name="held",
    )(value)


def expert_kernel(
    mine_ref, line_ref, gain_ref, first, second, others, gate_up, down, out_ref, inputs_ref, *, experts
):
    width, share = gate_up.shape[1], second.shape[1]
    deep, line = width // share, line_ref[0]
    blocks = [first[:, :share], second[...]] + [others[i] for i in range(deep - 2)]
    blocks = [block.astype(jnp.float32) for block in blocks]
    square = functools.reduce(lambda x, y: x + y, [block * block for block in blocks])
    root = lax.rsqrt(jnp.sum(square, axis=-1, keepdims=True) * (1.0 / width) + EPS)
    for b, block in enumerate(blocks):
        columns = pl.ds(pl.multiple_of(lax.rem(line + deep - b, deep) * share, 128), share)
        inputs_ref[:, columns] = (block * root * gain_ref[:, columns]).astype(jnp.bfloat16)
    inputs = inputs_ref[...]
    tail = first[:, share:].astype(jnp.float32)
    lanes = lax.broadcasted_iota(jnp.int32, tail.shape, 1)
    mine = mine_ref[0]
    scale = jnp.sum(
        jnp.where((lanes == mine) | (lanes == mine + experts), tail, 0.0), 1, keepdims=True
    )
    gate = jnp.dot(inputs, gate_up[0], preferred_element_type=jnp.float32)
    upper = jnp.dot(inputs, gate_up[1], preferred_element_type=jnp.float32)
    hidden = ((upper + 1.0) * gate * jax.nn.sigmoid(1.702 * gate)).astype(jnp.bfloat16)
    total = jnp.dot(hidden, down[...], preferred_element_type=jnp.float32)
    out_ref[...] = (total * scale).astype(out_ref.dtype)


def expert_rows(mine_at, line_at, gain, groups, weights, experts, out_type):
    count, (units, width) = groups[0].shape[0], weights[1].shape
    return pl.pallas_call(
        functools.partial(expert_kernel, experts=experts),
        out_shape=pltpu.VMEM((count, width), out_type),
        in_specs=[SCALARS] * 2 + [VECTORS] * 6,
        out_specs=VECTORS,
        scratch_shapes=[pltpu.VMEM((count, width), jnp.bfloat16)],
        cost_estimate=pl.CostEstimate(
            flops=6 * count * width * units,
            bytes_accessed=6 * width * units,
            transcendentals=count * units,
        ),
        compiler_params=pltpu.CompilerParams(vmem_limit_bytes=12 * 2**20),
        name="expert",
    )(mine_at, line_at, gain, *groups, *weights)


def resid_kernel(line_ref, *refs):
    blocks, out_ref = refs[:-1], refs[-1]
    deep, share, line = len(blocks), blocks[0].shape[2], line_ref[0]
    for b, block in enumerate(blocks):
        columns = pl.ds(pl.multiple_of(lax.rem(line + deep - b, deep) * share, 128), share)
        out_ref[:, columns] = block[(deep - b) % deep].astype(jnp.float32)


def resid_rows(line_at, blocks):
    deep, half, share = blocks[0].shape
    return pl.pallas_call(
        resid_kernel,
        out_shape=pltpu.VMEM((half, deep * share), jnp.float32),
        in_specs=[SCALARS] + [VECTORS] * deep,
        out_specs=VECTORS,
        cost_estimate=pl.CostEstimate(flops=1_000_000, bytes_accessed=10_000, transcendentals=0),
        compiler_params=pltpu.CompilerParams(vmem_limit_bytes=4 * 2**20),
        name="resid",
    )(line_at, *blocks)


def finish_kernel(own_ref, near_ref, over_ref, *refs, first, count):
    resid, outs = refs[:-count], refs[-count:]
    half = outs[0].shape[0]
    for n, out_ref in enumerate(outs):
        rows = pl.ds((first + n) * half, half)
        total = own_ref[rows, :] + near_ref[rows, :].astype(jnp.float32)
        total = total + over_ref[pl.ds(n * half, half), :].astype(jnp.float32)
        if first + n == 0:
            total = total + resid[0][...]
        out_ref[...] = total.astype(out_ref.dtype)


def finish(own, near_back, over, first, count, resid=()):
    half, width = over.shape[0] // count, over.shape[1]
    kinds = [jnp.float32 if first + n == 0 else jnp.bfloat16 for n in range(count)]
    return pl.pallas_call(
        functools.partial(finish_kernel, first=first, count=count),
        out_shape=[pltpu.VMEM((half, width), kind) for kind in kinds],
        in_specs=[VECTORS] * (3 + len(resid)),
        out_specs=[VECTORS] * count,
        cost_estimate=pl.CostEstimate(
            flops=500_000_000, bytes_accessed=1_000_000, transcendentals=0
        ),
        compiler_params=pltpu.CompilerParams(vmem_limit_bytes=8 * 2**20),
        name="finish",
    )(own, near_back, over, *resid)


PLANE = 4


def plane_perm(holders, stage):
    return [
        (2 * e + h, 2 * (e ^ (1 if h == stage else 2)) + h) for e in range(holders) for h in (0, 1)
    ]


def line_perm(holders, step):
    return [(e, (e + PLANE * step) % holders) for e in range(holders)]


def dense_plan(
    inputs, x_pre, x_dec, o_weight, norm_gain, expert_ids, route_logits, w_gate_up, w_down
):
    tokens_here, width = x_pre.shape[0] + x_dec.shape[0], x_pre.shape[1]
    holders = lax.axis_size("ep")
    experts = holders // 2
    deep = holders // PLANE
    place, core = lax.axis_index("ep"), lax.axis_index("hp")
    line, spot = place // PLANE, place % PLANE
    half = tokens_here // 2
    swap = [(0, 1), (1, 0)]
    far_first = range(deep - 1, 0, -1)
    where = [jnp.reshape(v, (1,)).astype(jnp.int32) for v in (line, core, spot, place // 2)]
    line_at, core_at, spot_at, mine_at = where

    def plane(value, stage):
        return lax.ppermute(value, ("ep", "hp"), plane_perm(holders, stage))

    def along(value, step):
        return lax.ppermute(value, "ep", line_perm(holders, step))

    def gather_line(value):
        got = {k: along(value, k) for k in far_first}
        return [value] + [got[k] for k in range(1, deep)]

    gate_up_here, down_here = w_gate_up[0], w_down[0]
    gate_up_there = lax.ppermute(gate_up_here, "hp", swap)
    down_there = lax.ppermute(down_here, "hp", swap)

    weights = pack(gate_up_here, gate_up_there, down_here, down_there)

    columns = o_weight.T
    beside = plane(columns, 0)
    across = plane(jnp.stack([columns, beside]), 1)

    attn_rows, pieces = start(where, inputs, x_pre, x_dec, expert_ids, route_logits, experts, deep)
    attn = gather_line(attn_rows)
    arrived = {k: along(pieces[k], k) for k in far_first}
    arrived[0] = pieces[0]
    pieces = [arrived[k] for k in range(deep)]
    kept, given = project(core_at, spot_at, attn, columns, beside, across)
    added = jnp.stack([piece[:, : kept.shape[2]] for piece in pieces]).astype(jnp.float32)
    summed = (kept + lax.ppermute(given, "hp", swap) + added).astype(jnp.bfloat16)
    blocks = gather_line(summed)

    def back_from_here(block, back):
        turned = [block[(c - back) % deep] for c in range(deep)]
        return jnp.concatenate(turned, axis=0)

    columns_of = [back_from_here(block, b) for b, block in enumerate(blocks)]
    tails = jnp.concatenate([piece[:, kept.shape[2] :] for piece in pieces], axis=0)
    groups = [
        jnp.concatenate([columns_of[0], tails], axis=1),
        columns_of[1],
        jnp.stack(columns_of[2:]),
    ]
    parts = range(len(groups))
    gain = held(norm_gain.reshape(1, width))

    def expert(groups, out_type):
        return expert_rows(mine_at, line_at, gain, groups, weights, experts, out_type)

    near_groups = [plane(groups[i], 0) for i in parts]
    both_groups = [plane(near_groups[i], 1) for i in parts]
    far_groups = [plane(groups[i], 1) for i in parts]
    own = expert(groups, jnp.float32)
    near_out = expert(near_groups, jnp.bfloat16)
    both_out = expert(both_groups, jnp.bfloat16)
    far_out = expert(far_groups, jnp.float32)
    far_back = plane(both_out, 0)
    near_back = plane(near_out, 0)
    low = deep // 2
    edge = low * half
    over_high = plane(
        (far_out[edge:] + far_back[edge:].astype(jnp.float32)).astype(jnp.bfloat16), 1
    )
    over_low = plane((far_out[:edge] + far_back[:edge].astype(jnp.float32)).astype(jnp.bfloat16), 1)
    sent = finish(own, near_back, over_high, low, deep - low)
    got = [along(block, deep - low - n) for n, block in enumerate(sent)]
    own_stream = resid_rows(line_at, blocks)
    rest, *sent = finish(own, near_back, over_low, 0, low, (own_stream,))
    got += [along(block, deep - 1 - n) for n, block in enumerate(sent)]
    for block in got:
        rest = rest + block.astype(jnp.float32)
    return rest.astype(jnp.bfloat16)


def on_device(
    x_pre,
    x_dec,
    prefill_query_rows,
    prefill_key_values,
    decode_query_rows,
    decode_key_values,
    cache,
    cache_len,
    sinks,
    o_weight,
    norm_gain,
    expert_ids,
    route_logits,
    w_gate_up,
    w_down,
):
    inputs = (
        prefill_query_rows,
        prefill_key_values,
        decode_query_rows,
        decode_key_values,
        cache,
        cache_len,
        sinks,
    )
    rest = (o_weight, norm_gain, expert_ids, route_logits, w_gate_up, w_down)
    tokens_here, topk = expert_ids.shape
    holders = lax.axis_size("ep")
    dense = tokens_here <= 2 * slot_count(tokens_here, topk, holders // 2)
    even = holders % PLANE == 0 and holders >= 3 * PLANE and x_pre.shape[1] % (holders // PLANE * 128) == 0
    if dense and even and lax.axis_size("hp") == 2:
        return dense_plan(inputs, x_pre, x_dec, *rest)
    return slot_plan(attention(*inputs), jnp.concatenate([x_pre, x_dec], axis=0), *rest)


def solution(mesh):
    placed = (
        P(("groups", "ep"), None),
        P(("groups", "ep"), None),
        P(("groups", "ep"), "hp"),
        P(None, ("groups", "ep"), "hp"),
        P(("groups", "ep"), "hp"),
        P(None, ("groups", "ep"), "hp"),
        P(None, ("groups", "ep"), None, "hp"),
        P(("groups", "ep")),
        P("hp"),
        P("hp", "ep"),
        P(),
        P(("groups", "ep"), None),
        P(("groups", "ep"), None),
        P("ep", None, None, "hp"),
        P("ep", "hp", None),
    )
    return jax.shard_map(
        on_device,
        mesh=mesh,
        in_specs=placed,
        out_specs=P(("groups", "ep", "hp"), None),
        check_vma=False,
    )
```
